32 devices in a mesh: strip: 32 (over z, y, x, core).
Axes of the slice: x: 2, y: 2, z: 4, core: 2. Of those that a mesh axis runs over, the one named last changes fastest.
Arguments:
- features: bfloat16 [64, 1024, 1024], P(None, 'strip'), may hold values from -6 to 6
- row_kernel: bfloat16 [8, 8, 8, 129], replicated, may hold values from -0.1875 to 0.1875
- mix_weight: bfloat16 [64, 64], replicated, may hold values from -0.75 to 0.75
- channel_bias: float32 [64], replicated, may hold values from -3 to 3
Outputs:
- layer_out: bfloat16 [64, 1024, 1024], P(None, 'strip')
The draws below stay inside these ranges and needn't reach their ends.
All inputs are finite; a program needn't handle non-finite values.
Results may differ from the reference program's by a relative error of at most 0.001.
Values may be sent and summed in bfloat16 or wider, within the bound.
A program may use at most 128 MiB of HBM per device.

```python
import jax
import jax.numpy as jnp
from jax import lax

C = 64
GW = 8
HALF = 64
ROWS_DEV = 32
NCOL = 1024
TAPS = 129
GROUPS = 8
ROWS = 1024
N_STRIP = 32


def block_scale(key, extent, split, smallest, largest):
    loudness, own = 1.0, jax.random.fold_in(key, 6)
    for position, shards_of in split:
        heights = jnp.exp(jax.random.uniform(jax.random.fold_in(own, position), (shards_of,), jnp.float32, smallest / len(split), largest / len(split)))
        loudness = loudness * jnp.repeat(heights, extent[position] // shards_of).reshape([-1 if axis == position else 1 for axis in range(len(extent))])
    return loudness


def bell_draw(own_key, dims, deviation, most, cuts=(), dtype=jnp.bfloat16):
    loudness = block_scale(own_key, dims, cuts, -0.22, 0.18) if cuts else 1.0
    drawn = jax.random.normal(own_key, dims, jnp.float32) * deviation * loudness
    return jnp.minimum(jnp.maximum(drawn, -most), most).astype(dtype)


def setup_inputs(seed: int = 0) -> dict:
    arg_keys = jax.random.split(jax.random.key(seed), 5)
    return {
        "features": bell_draw(arg_keys[0], (C, ROWS, NCOL), 1.0, 6.0, ((1, 32),)),
        "row_kernel": bell_draw(arg_keys[1], (GROUPS, GW, GW, TAPS), (GW * TAPS) ** -0.5, 0.1875),
        "mix_weight": bell_draw(arg_keys[2], (C, C), C ** -0.5, 0.75),
        "channel_bias": bell_draw(arg_keys[3], (C,), 0.5, 3.0, (), jnp.float32),
    }


def reference(features, row_kernel, mix_weight, channel_bias):
    grid_rows = ROWS_DEV * N_STRIP
    tap_count = 2 * HALF + 1
    front = row_kernel[..., HALF::-1]
    back = row_kernel[..., 2 * HALF:HALF:-1]
    middle = jnp.zeros((GROUPS, GW, GW, grid_rows - tap_count), jnp.bfloat16)
    filters = jnp.concatenate([front, middle, back], axis=-1).astype(jnp.float32)
    spectra = jnp.fft.rfft(filters, axis=-1)
    grouped = features.astype(jnp.float32).reshape(GROUPS, GW, grid_rows, NCOL)

    def one_group(pair):
        block, spectrum = pair
        block_hat = jnp.fft.rfft(block, axis=1)
        out_hat = jnp.einsum("oif,ifw->ofw", spectrum, block_hat)
        return jnp.fft.irfft(out_hat, n=grid_rows, axis=1)

    conv = lax.map(one_group, (grouped, spectra)).reshape(C, grid_rows, NCOL)
    mixed = jnp.einsum("io,irw->orw", mix_weight.astype(jnp.float32), features.astype(jnp.float32))
    total = conv + mixed + channel_bias[:, None, None]
    return jax.nn.gelu(total).astype(jnp.bfloat16)
```

```python
import functools

import jax
import jax.numpy as jnp
from jax import lax
from jax.experimental import pallas as pl
from jax.experimental.pallas import tpu as pltpu
from jax.sharding import PartitionSpec as P

MESH = pl.DeviceIdType.MESH
CORES = 2
PIECES = 2
AHEAD = 2


def kernel(
    chips,
    features,
    taps,
    mixes,
    bias,
    out,
    own,
    halo,
    weights,
    mixer,
    total,
    staged,
    own_sem,
    own_send,
    own_recv,
    near_send,
    near_recv,
    far_send,
    far_recv,
    out_sem,
    out_send,
    out_recv,
):
    channels, strip_rows, columns = features.shape
    groups, segments, width, lanes = taps.shape
    part = columns // CORES
    piece = part // PIECES
    block = width * strip_rows

    me = lax.axis_index("strip")
    chip, core = lax.div(me, CORES), lax.rem(me, CORES)
    odd = lax.rem(chip, 2)
    near_chip = chip + 1 - 2 * odd
    far_chip = lax.rem(chip + 2 + odd * (chips - 4), chips)
    back_chip = lax.rem(chip + (chips - 2) - odd * (chips - 4), chips)
    peer = chip * CORES + 1 - core
    far = far_chip * CORES + core
    back = back_chip * CORES + core

    def half(which):
        return pl.ds(pl.multiple_of(which * part, part), part)

    def group_rows(g):
        return pl.ds(pl.multiple_of(g * width, width), width)

    def own_load():
        return pltpu.make_async_copy(features.at[:, :, half(core)], own.at[core], own_sem)

    def own_swap():
        return pltpu.make_async_remote_copy(
            src_ref=features.at[:, :, half(1 - core)],
            dst_ref=own.at[core],
            send_sem=own_send,
            recv_sem=own_recv,
            device_id=(peer,),
            device_id_type=MESH,
        )

    def near_copy(g, q, target):
        return pltpu.make_async_remote_copy(
            src_ref=features.at[group_rows(g), :, pl.ds(target * part + q * piece, piece)],
            dst_ref=halo.at[odd, core, group_rows(g), :, pl.ds(q * piece, piece)],
            send_sem=near_send,
            recv_sem=near_recv.at[g, q, core],
            device_id=(near_chip * CORES + target,),
            device_id_type=MESH,
        )

    def near_wait(g, q, t):
        region = halo.at[1 - odd, t, group_rows(g), :, pl.ds(q * piece, piece)]
        pltpu.make_async_remote_copy(
            src_ref=region,
            dst_ref=region,
            send_sem=near_send,
            recv_sem=near_recv.at[g, q, t],
            device_id=(far,),
            device_id_type=MESH,
        ).wait_recv()

    def far_copy(g, q, t):
        return pltpu.make_async_remote_copy(
            src_ref=halo.at[1 - odd, t, group_rows(g), :, pl.ds(q * piece, piece)],
            dst_ref=halo.at[odd, t, group_rows(g), :, pl.ds(q * piece, piece)],
            send_sem=far_send,
            recv_sem=far_recv.at[g, q, t],
            device_id=(far,),
            device_id_type=MESH,
        )

    def send_near(g):
        for q in range(PIECES):
            for target in range(CORES):
                near_copy(g, q, target).start()

    def relay(g, q):
        for t in range(CORES):
            near_wait(g, q, t)
            far_copy(g, q, t).start()

    def build(g):
        shape = (strip_rows, 128)
        row = lax.broadcasted_iota(jnp.int32, shape, 0)
        lane = lax.rem(lax.broadcasted_iota(jnp.int32, shape, 1), strip_rows)
        inside = lane >= row
        same = lane == row
        for o in range(width):
            rows = pl.ds(o * strip_rows, strip_rows)
            for first in range(0, lanes, 128):
                before = jnp.zeros(shape, jnp.float32)
                for s in range(segments):
                    line = jnp.broadcast_to(taps[g, s, pl.ds(o, 1), pl.ds(first, 128)], shape)
                    here = pltpu.roll(line, 0, 1, stride=1, stride_axis=0)
                    weights[s, rows, pl.ds(first, 128)] = jnp.where(inside, here, before).astype(jnp.bfloat16)
                    before = pltpu.roll(line, 128 - strip_rows, 1, stride=1, stride_axis=0)
            for first in range(0, channels * strip_rows, 128):
                line = jnp.broadcast_to(mixes[g, pl.ds(o, 1), pl.ds(first, 128)], shape)
                mixer[rows, pl.ds(first, 128)] = jnp.where(same, line, 0.0).astype(jnp.bfloat16)

    def dot(a, b):
        return jnp.dot(a, b, preferred_element_type=jnp.float32)

    def inner(g):
        for q in range(PIECES):
            cols = pl.ds(q * piece, piece)
            for b in range(CORES):
                value = None
                for t in range(CORES):
                    term = dot(weights[t - b + 2], own[t, group_rows(g), :, cols].reshape(block, piece))
                    value = term if value is None else value + term
                for i in range(groups):
                    value += dot(
                        mixer[:, pl.ds(i * block, block)],
                        own[b, pl.ds(i * width, width), :, cols].reshape(block, piece),
                    )
                total[b, :, cols] = value

    def outer(g, q):
        cols = pl.ds(q * piece, piece)
        for t in range(CORES):
            far_copy(g, q, t).wait_recv()
        for b in range(CORES):
            value = total[b, :, cols]
            for role in range(2):
                for t in range(CORES):
                    s = t + (2 * CORES if role else 0) - b
                    if 0 <= s < segments:
                        value += dot(weights[s], halo[role, t, group_rows(g), :, cols].reshape(block, piece))
            for o in range(width):
                x = value[o * strip_rows : (o + 1) * strip_rows] + bias[g * width + o]
                staged[b, g * width + o, :, cols] = jax.nn.gelu(x).astype(jnp.bfloat16)
        place = pl.ds(pl.multiple_of(core * part + q * piece, piece), piece)
        pltpu.make_async_copy(
            staged.at[core, group_rows(g), :, cols], out.at[group_rows(g), :, place], out_sem
        ).start()
        pltpu.make_async_remote_copy(
            src_ref=staged.at[1 - core, group_rows(g), :, cols],
            dst_ref=out.at[group_rows(g), :, place],
            send_sem=out_send,
            recv_sem=out_recv,
            device_id=(peer,),
            device_id_type=MESH,
        ).start()

    own_load().start()
    barrier = pltpu.get_barrier_semaphore()
    friends = (peer, near_chip * CORES, near_chip * CORES + 1, far, back)
    for friend in friends:
        pl.semaphore_signal(barrier, inc=1, device_id=(friend,), device_id_type=MESH)
    pl.semaphore_wait(barrier, len(friends))

    for g in range(AHEAD):
        send_near(g)
    own_swap().start()
    own_load().wait()
    own_swap().wait_recv()

    def step(g, carry):
        @pl.when(g + AHEAD < groups)
        def _():
            send_near(g + AHEAD)

        relay(g, 0)

        @pl.when(g > 0)
        def _():
            for q in range(PIECES):
                outer(g - 1, q)

        for q in range(1, PIECES):
            relay(g, q)
        build(g)
        inner(g)
        return carry

    lax.fori_loop(0, groups, step, 0)
    for q in range(PIECES):
        outer(groups - 1, q)

    own_swap().wait_send()
    everything = pltpu.make_async_remote_copy(
        src_ref=features,
        dst_ref=features,
        send_sem=near_send,
        recv_sem=out_recv,
        device_id=(peer,),
        device_id_type=MESH,
    )
    everything.wait_send()
    pltpu.make_async_remote_copy(
        src_ref=halo.at[0],
        dst_ref=halo.at[1],
        send_sem=far_send,
        recv_sem=out_recv,
        device_id=(peer,),
        device_id_type=MESH,
    ).wait_send()
    pltpu.make_async_copy(staged.at[core], out.at[:, :, half(core)], out_sem).wait()
    swapped = pltpu.make_async_remote_copy(
        src_ref=staged.at[1 - core],
        dst_ref=out.at[:, :, half(1 - core)],
        send_sem=out_send,
        recv_sem=out_recv,
        device_id=(peer,),
        device_id_type=MESH,
    )
    swapped.wait_send()
    swapped.wait_recv()


def local(chips, features, row_kernel, mix_weight, channel_bias):
    channels, strip_rows, columns = features.shape
    groups, width, _, tap_count = row_kernel.shape
    assert tap_count - 1 == 2 * CORES * strip_rows
    segments = 2 * CORES + 1
    part = columns // CORES
    block = width * strip_rows
    taps = jnp.pad(row_kernel, ((0, 0), (0, 0), (0, 0), (0, segments * strip_rows - tap_count)))
    taps = taps.reshape(groups, width, width, segments, strip_rows)
    taps = taps.transpose(0, 3, 1, 2, 4).reshape(groups, segments, width, block)
    taps = taps.astype(jnp.float32)
    mixes = jnp.repeat(mix_weight.T.astype(jnp.float32), strip_rows, axis=1)
    mixes = mixes.reshape(groups, width, channels * strip_rows)
    dma = pltpu.SemaphoreType.DMA
    bf16 = features.dtype
    return pl.pallas_call(
        functools.partial(kernel, chips),
        name="layer",
        out_shape=jax.ShapeDtypeStruct(features.shape, bf16),
        in_specs=[
            pl.BlockSpec(memory_space=pl.ANY),
            pl.BlockSpec(memory_space=pltpu.VMEM),
            pl.BlockSpec(memory_space=pltpu.VMEM),
            pl.BlockSpec(memory_space=pltpu.SMEM),
        ],
        out_specs=pl.BlockSpec(memory_space=pl.ANY),
        scratch_shapes=[
            pltpu.VMEM((CORES, channels, strip_rows, part), bf16),
            pltpu.VMEM((2, CORES, channels, strip_rows, part), bf16),
            pltpu.VMEM((segments, block, block), bf16),
            pltpu.VMEM((block, channels * strip_rows), bf16),
            pltpu.VMEM((CORES, block, part), jnp.float32),
            pltpu.VMEM((CORES, channels, strip_rows, part), bf16),
            dma,
            dma,
            dma,
            dma,
            dma((groups, PIECES, CORES)),
            dma,
            dma((groups, PIECES, CORES)),
            dma,
            dma,
            dma,
        ],
        compiler_params=pltpu.CompilerParams(
            collective_id=0, has_side_effects=True, vmem_limit_bytes=48 * 1024 * 1024
        ),
    )(features, taps, mixes, channel_bias)


def solution(mesh):
    chips = mesh.shape["strip"] // CORES
    assert chips % 2 == 0 and chips >= 4
    return jax.shard_map(
        functools.partial(local, chips),
        mesh=mesh,
        in_specs=(P(None, "strip", None), P(), P(), P()),
        out_specs=P(None, "strip", None),
        check_vma=False,
    )
```

```python
import functools

import jax
import jax.numpy as jnp
from jax import lax
from jax.experimental import pallas as pl
from jax.experimental.pallas import tpu as pltpu
from jax.sharding import PartitionSpec as P

MESH = pl.DeviceIdType.MESH
CORES = 2
LANES = 128
PAIR = 2
AHEAD = 2


def kernel(
    chips,
    features,
    row_kernel,
    mix_weight,
    channel_bias,
    out,
    own,
    other,
    halo,
    raw,
    raw_mix,
    bias,
    spread,
    taps,
    mixes,
    weights,
    mixer,
    total,
    staged,
    load_sem,
    param_sem,
    own_send,
    own_recv,
    near_send,
    near_recv,
    far_send,
    far_recv,
    out_sem,
    out_send,
    out_recv,
):
    groups, width, strip_rows, columns = features.shape
    _, _, _, pieces, _, _, piece = halo.shape
    segments = weights.shape[1]
    tap_count = row_kernel.shape[1]
    part = columns // CORES
    block = width * strip_rows
    pairs = pieces // PAIR
    span = PAIR * piece

    me = lax.axis_index("strip")
    chip, core = lax.div(me, CORES), lax.rem(me, CORES)
    odd = lax.rem(chip, 2)
    near_chip = chip + 1 - 2 * odd
    far_chip = lax.rem(chip + 2 + odd * (chips - 4), chips)
    back_chip = lax.rem(chip + (chips - 2) - odd * (chips - 4), chips)
    peer = chip * CORES + 1 - core
    far = far_chip * CORES + core
    back = back_chip * CORES + core
    near = (near_chip * CORES + core, near_chip * CORES + 1 - core)

    def half(which):
        return pl.ds(pl.multiple_of(which * part, part), part)

    def load(g):
        for mine, which in ((own.at[core], core), (other, 1 - core)):
            for q in range(pieces):
                place = pl.ds(pl.multiple_of(which * part + q * piece, piece), piece)
                pltpu.make_async_copy(features.at[g, :, :, place], mine.at[g, q], load_sem.at[g]).start()

    def loaded(g):
        pltpu.make_async_copy(features.at[g], features.at[g], load_sem.at[g]).wait()

    def swap(g):
        return pltpu.make_async_remote_copy(
            src_ref=other.at[g],
            dst_ref=own.at[core, g],
            send_sem=own_send,
            recv_sem=own_recv,
            device_id=(peer,),
            device_id_type=MESH,
        )

    def near_copy(g, q, turn):
        return pltpu.make_async_remote_copy(
            src_ref=other.at[g, q] if turn else own.at[core, g, q],
            dst_ref=halo.at[odd, core, g, q],
            send_sem=near_send,
            recv_sem=near_recv.at[g, q, turn],
            device_id=(near[turn],),
            device_id_type=MESH,
        )

    def far_copy(g, q, turn):
        t = 1 - core if turn else core
        return pltpu.make_async_remote_copy(
            src_ref=halo.at[1 - odd, t, g, q],
            dst_ref=halo.at[odd, t, g, q],
            send_sem=far_send,
            recv_sem=far_recv.at[g, q, turn],
            device_id=(far,),
            device_id_type=MESH,
        )

    def near_wait(g, q, turn):
        region = halo.at[1 - odd, 1 - core if turn else core, g, q]
        pltpu.make_async_remote_copy(
            src_ref=region,
            dst_ref=region,
            send_sem=near_send,
            recv_sem=near_recv.at[g, q, turn],
            device_id=(far,),
            device_id_type=MESH,
        ).wait_recv()

    def send_near(g):
        for q in range(pieces):
            for turn in range(2):
                near_copy(g, q, turn).start()

    def relay(g, q):
        for turn in range(2):
            near_wait(g, q, turn)
            far_copy(g, q, turn).start()

    def dot(a, b):
        return jnp.dot(a, b, preferred_element_type=jnp.float32)

    def prepare():
        rows = groups * width
        raw_copy.wait()
        mix_copy.wait()
        bias_copy.wait()
        spread[...] = jnp.zeros_like(spread)
        for page in range(spread.shape[0]):
            size = min(LANES, tap_count - page * LANES)
            spread[page, :, pl.ds(0, size)] = raw[:, pl.ds(page * LANES, size)].astype(jnp.float32)
        fit = LANES // strip_rows
        lane = lax.broadcasted_iota(jnp.int32, (rows, LANES), 1)
        for first in range(0, width, fit):
            for s in range(segments):
                line = jnp.zeros((rows, LANES), jnp.float32)
                for n in range(fit):
                    source = pl.ds(first + n, rows, stride=width)
                    part_line = spread[s * strip_rows // LANES, source, :]
                    shift = (n * strip_rows - s * strip_rows) % LANES
                    part_line = pltpu.roll(part_line, shift, 1) if shift else part_line
                    line = jnp.where(lane // strip_rows == n, part_line, line)
                taps[s, :, :, pl.ds(first * strip_rows, LANES)] = line.reshape(groups, width, LANES)
        shape = (rows, rows * strip_rows)
        pick = lax.broadcasted_iota(jnp.int32, shape, 1) // strip_rows == lax.broadcasted_iota(jnp.int32, shape, 0)
        expanded = lax.dot_general(
            raw_mix[...],
            pick.astype(raw_mix.dtype),
            (((0,), (0,)), ((), ())),
            preferred_element_type=jnp.float32,
        )
        mixes[...] = expanded.reshape(mixes.shape)

    def build(g):
        slot = lax.rem(g, 2)
        shape = (strip_rows, LANES)
        row = lax.broadcasted_iota(jnp.int32, shape, 0)
        lane = lax.rem(lax.broadcasted_iota(jnp.int32, shape, 1), strip_rows)
        inside = lane >= row
        same = lane == row
        for o in range(width):
            rows = pl.ds(o * strip_rows, strip_rows)
            source = pl.ds(o, 1)
            for first in range(0, block, LANES):
                before = jnp.zeros(shape, jnp.float32)
                for s in range(segments):
                    line = jnp.broadcast_to(taps[s, g, source, pl.ds(first, LANES)], shape)
                    here = pltpu.roll(line, 0, 1, stride=1, stride_axis=0)
                    weights[lax.rem(g, 3), s, rows, pl.ds(first, LANES)] = jnp.where(inside, here, before).astype(jnp.bfloat16)
                    before = pltpu.roll(line, LANES - strip_rows, 1, stride=1, stride_axis=0)
            for first in range(0, groups * block, LANES):
                line = jnp.broadcast_to(mixes[g, source, pl.ds(first, LANES)], shape)
                mixer[rows, pl.ds(first, LANES)] = jnp.where(same, line, 0.0).astype(jnp.bfloat16)

    def wide(ref, n):
        return jnp.concatenate([ref[n * PAIR + k].reshape(block, piece) for k in range(PAIR)], axis=1)

    def inner(g):
        slot = lax.rem(g, 2)
        for n in range(pairs):
            for b in range(CORES):
                value = None
                for t in range(CORES):
                    term = dot(weights[lax.rem(g, 3), t - b + CORES], wide(own.at[t, g], n))
                    value = term if value is None else value + term
                for i in range(groups):
                    value += dot(mixer[:, pl.ds(i * block, block)], wide(own.at[b, i], n))
                total[slot, b, :, pl.ds(n * span, span)] = value

    def outer(g, n):
        slot = lax.rem(g, 2)
        cols = pl.ds(n * span, span)
        for q in range(n * PAIR, (n + 1) * PAIR):
            for turn in range(2):
                far_copy(g, q, turn).wait_recv()
        for b in range(CORES):
            value = total[slot, b, :, cols]
            for role in range(2):
                for t in range(CORES):
                    s = t + (2 * CORES if role else 0) - b
                    if 0 <= s < segments:
                        value += dot(weights[lax.rem(g, 3), s], wide(halo.at[role, t, g], n))
            for o in range(width):
                x = value[o * strip_rows : (o + 1) * strip_rows] + bias[g * width + o]
                staged[b, g, o, :, cols] = jax.nn.gelu(x).astype(jnp.bfloat16)
        place = pl.ds(pl.multiple_of(core * part + n * span, span), span)
        pltpu.make_async_copy(staged.at[core, g, :, :, cols], out.at[g, :, :, place], out_sem).start()
        pltpu.make_async_remote_copy(
            src_ref=staged.at[1 - core, g, :, :, cols],
            dst_ref=out.at[g, :, :, place],
            send_sem=out_send,
            recv_sem=out_recv,
            device_id=(peer,),
            device_id_type=MESH,
        ).start()

    for g in range(AHEAD):
        load(g)
    barrier = pltpu.get_barrier_semaphore()
    friends = (peer, *near, far, back)
    for friend in friends:
        pl.semaphore_signal(barrier, inc=1, device_id=(friend,), device_id_type=MESH)
    raw_copy = pltpu.make_async_copy(row_kernel, raw, param_sem.at[0])
    mix_copy = pltpu.make_async_copy(mix_weight, raw_mix, param_sem.at[1])
    bias_copy = pltpu.make_async_copy(channel_bias, bias, param_sem.at[2])
    for g in range(AHEAD, groups):
        load(g)
    raw_copy.start()
    mix_copy.start()
    bias_copy.start()
    pl.semaphore_wait(barrier, len(friends))

    for g in range(AHEAD):
        loaded(g)
        send_near(g)
        swap(g).start()
    for g in range(AHEAD, groups):
        loaded(g)
        swap(g).start()
    prepare()
    pltpu.make_async_remote_copy(
        src_ref=other,
        dst_ref=own.at[1 - core],
        send_sem=own_send,
        recv_sem=own_recv,
        device_id=(peer,),
        device_id_type=MESH,
    ).wait_recv()

    def step(g, carry):
        @pl.when(g + AHEAD < groups)
        def _():
            send_near(g + AHEAD)

        relay(g, 0)

        @pl.when(g == 0)
        def _():
            build(g)
            inner(g)

        @pl.when(g + 1 < groups)
        def _():
            build(g + 1)

        relay(g, 1)

        @pl.when(g > 0)
        def _():
            outer(g - 1, 1)

        relay(g, 2)

        @pl.when(g + 1 < groups)
        def _():
            inner(g + 1)

        relay(g, 3)
        outer(g, 0)
        return carry

    lax.fori_loop(0, groups, step, 0)
    outer(groups - 1, 1)

    def sent(ref, sem):
        pltpu.make_async_remote_copy(
            src_ref=ref,
            dst_ref=ref,
            send_sem=sem,
            recv_sem=out_recv,
            device_id=(peer,),
            device_id_type=MESH,
        ).wait_send()

    sent(other, own_send)
    sent(features, near_send)
    sent(halo.at[0], far_send)
    pltpu.make_async_copy(staged.at[core], out.at[:, :, :, half(core)], out_sem).wait()
    swapped = pltpu.make_async_remote_copy(
        src_ref=staged.at[1 - core],
        dst_ref=out.at[:, :, :, half(1 - core)],
        send_sem=out_send,
        recv_sem=out_recv,
        device_id=(peer,),
        device_id_type=MESH,
    )
    swapped.wait_send()
    swapped.wait_recv()


def fixed(array):
    return pltpu.with_memory_space_constraint(array, pltpu.HBM)


def local(chips, features, row_kernel, mix_weight, channel_bias):
    channels, strip_rows, columns = features.shape
    groups, width, _, tap_count = row_kernel.shape
    assert tap_count - 1 == 2 * CORES * strip_rows and LANES % strip_rows == 0
    segments = 2 * CORES + 1
    part = columns // CORES
    block = width * strip_rows
    pieces = part // LANES
    assert pieces == 4
    dma = pltpu.SemaphoreType.DMA
    bf16 = features.dtype
    shape = (groups, width, strip_rows, columns)
    buffer = (groups, pieces, width, strip_rows, LANES)
    anywhere = pl.BlockSpec(memory_space=pl.ANY)
    out = pl.pallas_call(
        functools.partial(kernel, chips),
        name="layer",
        out_shape=jax.ShapeDtypeStruct(shape, bf16),
        in_specs=[pl.BlockSpec(memory_space=pltpu.HBM)] * 4,
        out_specs=anywhere,
        scratch_shapes=[
            pltpu.VMEM((CORES, *buffer), bf16),
            pltpu.VMEM(buffer, bf16),
            pltpu.VMEM((2, CORES, *buffer), bf16),
            pltpu.VMEM((channels * width, tap_count), row_kernel.dtype),
            pltpu.VMEM((channels, channels), mix_weight.dtype),
            pltpu.SMEM((channels,), channel_bias.dtype),
            pltpu.VMEM((pl.cdiv(tap_count, LANES), channels * width, LANES), jnp.float32),
            pltpu.VMEM((segments, groups, width, block), jnp.float32),
            pltpu.VMEM((groups, width, channels * strip_rows), jnp.float32),
            pltpu.VMEM((3, segments, block, block), bf16),
            pltpu.VMEM((block, channels * strip_rows), bf16),
            pltpu.VMEM((2, CORES, block, part), jnp.float32),
            pltpu.VMEM((CORES, groups, width, strip_rows, part), bf16),
            dma((groups,)),
            dma((3,)),
            dma,
            dma,
            dma,
            dma((groups, pieces, CORES)),
            dma,
            dma((groups, pieces, CORES)),
            dma,
            dma,
            dma,
        ],
        compiler_params=pltpu.CompilerParams(
            collective_id=0, has_side_effects=True, vmem_limit_bytes=48 * 1024 * 1024
        ),
    )(
        features.reshape(shape),
        fixed(row_kernel.reshape(channels * width, tap_count)),
        fixed(mix_weight),
        fixed(channel_bias),
    )
    return out.reshape(features.shape)


def solution(mesh):
    chips = mesh.shape["strip"] // CORES
    assert chips % 2 == 0 and chips >= 4
    return jax.shard_map(
        functools.partial(local, chips),
        mesh=mesh,
        in_specs=(P(None, "strip", None), P(), P(), P()),
        out_specs=P(None, "strip", None),
        check_vma=False,
    )
```

```python
import functools

import jax
import jax.numpy as jnp
from jax import lax
from jax.experimental import pallas as pl
from jax.experimental.pallas import tpu as pltpu
from jax.sharding import PartitionSpec as P

MESH = pl.DeviceIdType.MESH
CORES = 2
LANES = 128
PAIR = 2
AHEAD = 2


def kernel(
    chips,
    features,
    row_kernel,
    mix_weight,
    channel_bias,
    out,
    own,
    other,
    halo,
    raw,
    raw_mix,
    bias,
    spread,
    taps,
    mixes,
    weights,
    mixer,
    total,
    staged,
    stage,
    load_sem,
    param_sem,
    own_send,
    own_recv,
    near_send,
    near_recv,
    far_send,
    far_recv,
    out_sem,
    out_send,
    out_recv,
    hop_send,
    hop_recv,
    ready,
):
    groups, width, strip_rows, columns = features.shape
    _, _, _, pieces, _, _, piece = halo.shape
    segments = weights.shape[1]
    tap_count = row_kernel.shape[1]
    part = columns // CORES
    block = width * strip_rows
    pairs = pieces // PAIR
    span = PAIR * piece

    me = lax.axis_index("strip")
    chip, core = lax.div(me, CORES), lax.rem(me, CORES)
    odd = lax.rem(chip, 2)
    near_chip = chip + 1 - 2 * odd
    far_chip = lax.rem(chip + 2 + odd * (chips - 4), chips)
    back_chip = lax.rem(chip + (chips - 2) - odd * (chips - 4), chips)
    peer = chip * CORES + 1 - core
    far = far_chip * CORES + core
    near = (near_chip * CORES + core, near_chip * CORES + 1 - core)
    back = (back_chip * CORES + core, back_chip * CORES + 1 - core)
    up_chip = lax.rem(chip + 2, chips)
    down_chip = lax.rem(chip + chips - 2, chips)
    last = (groups - 1, pieces - 1)

    def half(which):
        return pl.ds(pl.multiple_of(which * part, part), part)

    def load(g):
        for mine, which in ((own.at[core], core), (other, 1 - core)):
            for q in range(pieces):
                place = pl.ds(pl.multiple_of(which * part + q * piece, piece), piece)
                pltpu.make_async_copy(features.at[g, :, :, place], mine.at[g, q], load_sem.at[g]).start()

    def loaded(g):
        pltpu.make_async_copy(features.at[g], features.at[g], load_sem.at[g]).wait()

    def swap(g):
        return pltpu.make_async_remote_copy(
            src_ref=other.at[g],
            dst_ref=own.at[core, g],
            send_sem=own_send,
            recv_sem=own_recv,
            device_id=(peer,),
            device_id_type=MESH,
        )

    def near_copy(g, q, turn):
        return pltpu.make_async_remote_copy(
            src_ref=other.at[g, q] if turn else own.at[core, g, q],
            dst_ref=halo.at[odd, core, g, q],
            send_sem=near_send,
            recv_sem=near_recv.at[g, q, turn],
            device_id=(near[turn],),
            device_id_type=MESH,
        )

    def far_copy(g, q, turn):
        t = 1 - core if turn else core
        return pltpu.make_async_remote_copy(
            src_ref=halo.at[1 - odd, t, g, q],
            dst_ref=halo.at[odd, t, g, q],
            send_sem=far_send,
            recv_sem=far_recv.at[g, q, turn],
            device_id=(far,),
            device_id_type=MESH,
        )

    def near_wait(g, q, turn):
        region = halo.at[1 - odd, 1 - core if turn else core, g, q]
        pltpu.make_async_remote_copy(
            src_ref=region,
            dst_ref=region,
            send_sem=near_send,
            recv_sem=near_recv.at[g, q, turn],
            device_id=(far,),
            device_id_type=MESH,
        ).wait_recv()

    def hop_copy(turn):
        return pltpu.make_async_remote_copy(
            src_ref=other.at[last] if turn else own.at[core, *last],
            dst_ref=stage.at[turn],
            send_sem=hop_send,
            recv_sem=hop_recv.at[turn],
            device_id=(back[turn],),
            device_id_type=MESH,
        )

    def hop_forward(turn):
        return pltpu.make_async_remote_copy(
            src_ref=stage.at[turn],
            dst_ref=halo.at[1 - odd, 1 - core if turn else core, *last],
            send_sem=far_send,
            recv_sem=far_recv.at[*last, turn],
            device_id=(near[0],),
            device_id_type=MESH,
        )

    def send_near(g):
        for q in range(pieces):
            for turn in range(2):
                near_copy(g, q, turn).start()

    def relay(g, q):
        for turn in range(2):
            near_wait(g, q, turn)
            if q < last[1]:
                far_copy(g, q, turn).start()
            else:
                pl.when(g < last[0])(far_copy(g, q, turn).start)

    def dot(a, b):
        return jnp.dot(a, b, preferred_element_type=jnp.float32)

    def prepare():
        rows = groups * width
        raw_copy.wait()
        mix_copy.wait()
        bias_copy.wait()
        spread[...] = jnp.zeros_like(spread)
        for page in range(spread.shape[0]):
            size = min(LANES, tap_count - page * LANES)
            spread[page, :, pl.ds(0, size)] = raw[:, pl.ds(page * LANES, size)].astype(jnp.float32)
        fit = LANES // strip_rows
        lane = lax.broadcasted_iota(jnp.int32, (rows, LANES), 1)
        for first in range(0, width, fit):
            for s in range(segments):
                line = jnp.zeros((rows, LANES), jnp.float32)
                for n in range(fit):
                    source = pl.ds(first + n, rows, stride=width)
                    part_line = spread[s * strip_rows // LANES, source, :]
                    shift = (n * strip_rows - s * strip_rows) % LANES
                    part_line = pltpu.roll(part_line, shift, 1) if shift else part_line
                    line = jnp.where(lane // strip_rows == n, part_line, line)
                taps[s, :, :, pl.ds(first * strip_rows, LANES)] = line.reshape(groups, width, LANES)
        shape = (rows, rows * strip_rows)
        pick = lax.broadcasted_iota(jnp.int32, shape, 1) // strip_rows == lax.broadcasted_iota(jnp.int32, shape, 0)
        expanded = lax.dot_general(
            raw_mix[...],
            pick.astype(raw_mix.dtype),
            (((0,), (0,)), ((), ())),
            preferred_element_type=jnp.float32,
        )
        mixes[...] = expanded.reshape(mixes.shape)

    def build(g):
        slot = lax.rem(g, 2)
        shape = (strip_rows, LANES)
        row = lax.broadcasted_iota(jnp.int32, shape, 0)
        lane = lax.rem(lax.broadcasted_iota(jnp.int32, shape, 1), strip_rows)
        inside = lane >= row
        same = lane == row
        for o in range(width):
            rows = pl.ds(o * strip_rows, strip_rows)
            source = pl.ds(o, 1)
            for first in range(0, block, LANES):
                before = jnp.zeros(shape, jnp.float32)
                for s in range(segments):
                    line = jnp.broadcast_to(taps[s, g, source, pl.ds(first, LANES)], shape)
                    here = pltpu.roll(line, 0, 1, stride=1, stride_axis=0)
                    weights[lax.rem(g, 3), s, rows, pl.ds(first, LANES)] = jnp.where(inside, here, before).astype(jnp.bfloat16)
                    before = pltpu.roll(line, LANES - strip_rows, 1, stride=1, stride_axis=0)
            for first in range(0, groups * block, LANES):
                line = jnp.broadcast_to(mixes[g, source, pl.ds(first, LANES)], shape)
                mixer[rows, pl.ds(first, LANES)] = jnp.where(same, line, 0.0).astype(jnp.bfloat16)

    def wide(ref, first, count):
        return jnp.concatenate([ref[first + k].reshape(block, piece) for k in range(count)], axis=1)

    def inner(g):
        slot = lax.rem(g, 2)
        for n in range(pairs):
            for b in range(CORES):
                value = None
                for t in range(CORES):
                    term = dot(weights[lax.rem(g, 3), t - b + CORES], wide(own.at[t, g], n * PAIR, PAIR))
                    value = term if value is None else value + term
                for i in range(groups):
                    value += dot(mixer[:, pl.ds(i * block, block)], wide(own.at[b, i], n * PAIR, PAIR))
                total[slot, b, :, pl.ds(n * span, span)] = value

    def outer(g, first, count):
        slot = lax.rem(g, 2)
        cols = pl.ds(first * piece, count * piece)
        for q in range(first, first + count):
            for turn in range(2):
                far_copy(g, q, turn).wait_recv()
        for b in range(CORES):
            value = total[slot, b, :, cols]
            for role in range(2):
                for t in range(CORES):
                    s = t + (2 * CORES if role else 0) - b
                    if 0 <= s < segments:
                        value += dot(weights[lax.rem(g, 3), s], wide(halo.at[role, t, g], first, count))
            for o in range(width):
                x = value[o * strip_rows : (o + 1) * strip_rows] + bias[g * width + o]
                staged[b, g, o, :, cols] = jax.nn.gelu(x).astype(jnp.bfloat16)
        place = pl.ds(pl.multiple_of(core * part + first * piece, piece), count * piece)
        pltpu.make_async_copy(staged.at[core, g, :, :, cols], out.at[g, :, :, place], out_sem).start()
        pltpu.make_async_remote_copy(
            src_ref=staged.at[1 - core, g, :, :, cols],
            dst_ref=out.at[g, :, :, place],
            send_sem=out_send,
            recv_sem=out_recv,
            device_id=(peer,),
            device_id_type=MESH,
        ).start()

    load(0)
    load(groups - 1)
    barrier = pltpu.get_barrier_semaphore()
    close = (*near, peer, down_chip * CORES, down_chip * CORES + 1)
    above = (up_chip * CORES, up_chip * CORES + 1)
    for friend in close:
        pl.semaphore_signal(barrier, inc=1, device_id=(friend,), device_id_type=MESH)

    @pl.when(chip < chips - 2)
    def _():
        for friend in above:
            pl.semaphore_signal(barrier, inc=1, device_id=(friend,), device_id_type=MESH)

    raw_copy = pltpu.make_async_copy(row_kernel, raw, param_sem.at[0])
    mix_copy = pltpu.make_async_copy(mix_weight, raw_mix, param_sem.at[1])
    bias_copy = pltpu.make_async_copy(channel_bias, bias, param_sem.at[2])
    for g in range(1, groups - 1):
        load(g)
    raw_copy.start()
    mix_copy.start()
    bias_copy.start()
    pl.semaphore_wait(barrier, len(close) + len(above) * jnp.minimum(lax.div(chip, 2), 1))

    @pl.when(chip >= chips - 2)
    def _():
        for friend in above:
            pl.semaphore_signal(ready, inc=1, device_id=(friend,), device_id_type=MESH)


    def hop():
        for turn in range(2):
            hop_copy(turn).start()

    loaded(0)
    send_near(0)
    loaded(groups - 1)
    pl.when(chip > 0)(hop)
    for g in range(1, AHEAD):
        loaded(g)
        send_near(g)
    for g in range(AHEAD, groups - 1):
        loaded(g)
    for g in range(groups):
        swap(g).start()
    prepare()
    pltpu.make_async_remote_copy(
        src_ref=other,
        dst_ref=own.at[1 - core],
        send_sem=own_send,
        recv_sem=own_recv,
        device_id=(peer,),
        device_id_type=MESH,
    ).wait_recv()

    @pl.when(chip == 1)
    def _():
        pl.semaphore_wait(ready, len(above))

    def step(g, carry):
        @pl.when((g == 1) & (chip == 0))
        def _():
            pl.semaphore_wait(ready, len(above))
            hop()

        @pl.when(g == groups - 1)
        def _():
            for turn in range(2):
                hop_copy(turn).wait_recv()
                hop_forward(turn).start()

        @pl.when(g + AHEAD < groups)
        def _():
            send_near(g + AHEAD)

        relay(g, 0)

        @pl.when(g == 0)
        def _():
            build(g)
            inner(g)

        @pl.when(g + 1 < groups)
        def _():
            build(g + 1)

        relay(g, 1)

        @pl.when(g > 0)
        def _():
            outer(g - 1, PAIR, PAIR)

        relay(g, 2)

        @pl.when(g + 1 < groups)
        def _():
            inner(g + 1)

        relay(g, 3)
        outer(g, 0, PAIR)
        return carry

    lax.fori_loop(0, groups, step, 0)
    for q in reversed(range(PAIR, pieces)):
        outer(groups - 1, q, 1)

    def sent(ref, sem):
        pltpu.make_async_remote_copy(
            src_ref=ref,
            dst_ref=ref,
            send_sem=sem,
            recv_sem=out_recv,
            device_id=(peer,),
            device_id_type=MESH,
        ).wait_send()

    sent(other, own_send)
    sent(features, near_send)
    sent(halo.at[0], far_send)
    sent(stage, hop_send)
    pltpu.make_async_copy(staged.at[core], out.at[:, :, :, half(core)], out_sem).wait()
    swapped = pltpu.make_async_remote_copy(
        src_ref=staged.at[1 - core],
        dst_ref=out.at[:, :, :, half(1 - core)],
        send_sem=out_send,
        recv_sem=out_recv,
        device_id=(peer,),
        device_id_type=MESH,
    )
    swapped.wait_send()
    swapped.wait_recv()


def fixed(array):
    return pltpu.with_memory_space_constraint(array, pltpu.HBM)


def local(chips, features, row_kernel, mix_weight, channel_bias):
    channels, strip_rows, columns = features.shape
    groups, width, _, tap_count = row_kernel.shape
    assert tap_count - 1 == 2 * CORES * strip_rows and LANES % strip_rows == 0
    segments = 2 * CORES + 1
    part = columns // CORES
    block = width * strip_rows
    pieces = part // LANES
    assert pieces == 4
    dma = pltpu.SemaphoreType.DMA
    bf16 = features.dtype
    shape = (groups, width, strip_rows, columns)
    buffer = (groups, pieces, width, strip_rows, LANES)
    anywhere = pl.BlockSpec(memory_space=pl.ANY)
    out = pl.pallas_call(
        functools.partial(kernel, chips),
        name="layer",
        out_shape=jax.ShapeDtypeStruct(shape, bf16),
        in_specs=[pl.BlockSpec(memory_space=pltpu.HBM)] * 4,
        out_specs=anywhere,
        scratch_shapes=[
            pltpu.VMEM((CORES, *buffer), bf16),
            pltpu.VMEM(buffer, bf16),
            pltpu.VMEM((2, CORES, *buffer), bf16),
            pltpu.VMEM((channels * width, tap_count), row_kernel.dtype),
            pltpu.VMEM((channels, channels), mix_weight.dtype),
            pltpu.SMEM((channels,), channel_bias.dtype),
            pltpu.VMEM((pl.cdiv(tap_count, LANES), channels * width, LANES), jnp.float32),
            pltpu.VMEM((segments, groups, width, block), jnp.float32),
            pltpu.VMEM((groups, width, channels * strip_rows), jnp.float32),
            pltpu.VMEM((3, segments, block, block), bf16),
            pltpu.VMEM((block, channels * strip_rows), bf16),
            pltpu.VMEM((2, CORES, block, part), jnp.float32),
            pltpu.VMEM((CORES, groups, width, strip_rows, part), bf16),
            pltpu.VMEM((2, width, strip_rows, LANES), bf16),
            dma((groups,)),
            dma((3,)),
            dma,
            dma,
            dma,
            dma((groups, pieces, CORES)),
            dma,
            dma((groups, pieces, CORES)),
            dma,
            dma,
            dma,
            dma,
            dma((2,)),
            pltpu.SemaphoreType.REGULAR,
        ],
        compiler_params=pltpu.CompilerParams(
            collective_id=0, has_side_effects=True, vmem_limit_bytes=48 * 1024 * 1024
        ),
    )(
        features.reshape(shape),
        fixed(row_kernel.reshape(channels * width, tap_count)),
        fixed(mix_weight),
        fixed(channel_bias),
    )
    return out.reshape(features.shape)


def solution(mesh):
    chips = mesh.shape["strip"] // CORES
    assert chips % 2 == 0 and chips >= 4
    return jax.shard_map(
        functools.partial(local, chips),
        mesh=mesh,
        in_specs=(P(None, "strip", None), P(), P(), P()),
        out_specs=P(None, "strip", None),
        check_vma=False,
    )
```

```python
import functools

import jax
import jax.numpy as jnp
from jax import lax
from jax.experimental import pallas as pl
from jax.experimental.pallas import tpu as pltpu
from jax.sharding import PartitionSpec as P

MESH = pl.DeviceIdType.MESH
CORES = 2
LANES = 128
PAIR = 2
AHEAD = 2


def kernel(
    chips,
    features,
    row_kernel,
    mix_weight,
    channel_bias,
    out,
    own,
    other,
    halo,
    raw,
    raw_mix,
    bias,
    spread,
    taps,
    mixes,
    weights,
    mixer,
    total,
    staged,
    stage,
    stage_wrap,
    load_sem,
    param_sem,
    own_send,
    own_recv,
    near_send,
    near_recv,
    far_send,
    far_recv,
    out_sem,
    out_send,
    out_recv,
    hop_send,
    hop_recv,
    ready,
    ready_wrap,
    late_send,
    wrap_send,
    wrap_recv,
    wrap_pass,
    wrap_done,
):
    groups, width, strip_rows, columns = features.shape
    _, _, _, pieces, _, _, piece = halo.shape
    segments = weights.shape[1]
    tap_count = row_kernel.shape[1]
    part = columns // CORES
    block = width * strip_rows
    pairs = pieces // PAIR
    span = PAIR * piece

    me = lax.axis_index("strip")
    chip, core = lax.div(me, CORES), lax.rem(me, CORES)
    odd = lax.rem(chip, 2)
    near_chip = chip + 1 - 2 * odd
    far_chip = lax.rem(chip + 2 + odd * (chips - 4), chips)
    back_chip = lax.rem(chip + (chips - 2) - odd * (chips - 4), chips)
    peer = chip * CORES + 1 - core
    far = far_chip * CORES + core
    near = (near_chip * CORES + core, near_chip * CORES + 1 - core)
    back = (back_chip * CORES + core, back_chip * CORES + 1 - core)
    up_chip = lax.rem(chip + 2, chips)
    down_chip = lax.rem(chip + chips - 2, chips)
    last = (groups - 1, pieces - 1)
    late = (groups - 1, pieces - 2)
    front = pl.ds(0, width // 2)
    rear = pl.ds(width // 2, width // 2)

    def half(which):
        return pl.ds(pl.multiple_of(which * part, part), part)

    def load(g):
        for mine, which in ((own.at[core], core), (other, 1 - core)):
            for q in range(pieces):
                place = pl.ds(pl.multiple_of(which * part + q * piece, piece), piece)
                pltpu.make_async_copy(features.at[g, :, :, place], mine.at[g, q], load_sem.at[g]).start()

    def loaded(g):
        pltpu.make_async_copy(features.at[g], features.at[g], load_sem.at[g]).wait()

    def swap(g):
        return pltpu.make_async_remote_copy(
            src_ref=other.at[g],
            dst_ref=own.at[core, g],
            send_sem=own_send,
            recv_sem=own_recv,
            device_id=(peer,),
            device_id_type=MESH,
        )

    def near_copy(g, q, turn):
        return pltpu.make_async_remote_copy(
            src_ref=other.at[g, q] if turn else own.at[core, g, q],
            dst_ref=halo.at[odd, core, g, q],
            send_sem=near_send,
            recv_sem=near_recv.at[g, q, turn],
            device_id=(near[turn],),
            device_id_type=MESH,
        )

    def far_copy(g, q, turn):
        t = 1 - core if turn else core
        return pltpu.make_async_remote_copy(
            src_ref=halo.at[1 - odd, t, g, q],
            dst_ref=halo.at[odd, t, g, q],
            send_sem=far_send.at[g],
            recv_sem=far_recv.at[g, q, turn],
            device_id=(far,),
            device_id_type=MESH,
        )

    def near_wait(g, q, turn):
        region = halo.at[1 - odd, 1 - core if turn else core, g, q]
        pltpu.make_async_remote_copy(
            src_ref=region,
            dst_ref=region,
            send_sem=near_send,
            recv_sem=near_recv.at[g, q, turn],
            device_id=(far,),
            device_id_type=MESH,
        ).wait_recv()

    def hop_copy(turn):
        return pltpu.make_async_remote_copy(
            src_ref=other.at[last] if turn else own.at[core, *last],
            dst_ref=stage.at[turn],
            send_sem=hop_send,
            recv_sem=hop_recv.at[turn],
            device_id=(back[turn],),
            device_id_type=MESH,
        )

    def hop_forward(turn):
        return pltpu.make_async_remote_copy(
            src_ref=stage.at[turn],
            dst_ref=halo.at[1 - odd, 1 - core if turn else core, *last],
            send_sem=far_send.at[last[0]],
            recv_sem=far_recv.at[*last, turn],
            device_id=(near[0],),
            device_id_type=MESH,
        )

    def late_copy(turn, part_rows):
        t = 1 - core if turn else core
        return pltpu.make_async_remote_copy(
            src_ref=halo.at[1 - odd, t, *late, part_rows],
            dst_ref=halo.at[odd, t, *late, part_rows],
            send_sem=late_send,
            recv_sem=far_recv.at[*late, turn],
            device_id=(far,),
            device_id_type=MESH,
        )

    def wrap_copy(turn):
        return pltpu.make_async_remote_copy(
            src_ref=other.at[*late, front] if turn else own.at[core, *late, front],
            dst_ref=stage_wrap.at[turn],
            send_sem=wrap_send,
            recv_sem=wrap_recv.at[turn],
            device_id=(back[turn],),
            device_id_type=MESH,
        )

    def wrap_forward(turn):
        return pltpu.make_async_remote_copy(
            src_ref=stage_wrap.at[turn],
            dst_ref=halo.at[1 - odd, 1 - core if turn else core, *late, front],
            send_sem=wrap_pass,
            recv_sem=wrap_done.at[turn],
            device_id=(near[0],),
            device_id_type=MESH,
        )

    def wrap_arrived(turn):
        region = halo.at[odd, 1 - core if turn else core, *late, front]
        pltpu.make_async_remote_copy(
            src_ref=region,
            dst_ref=region,
            send_sem=wrap_pass,
            recv_sem=wrap_done.at[turn],
            device_id=(near[0],),
            device_id_type=MESH,
        ).wait_recv()

    def send_near(g):
        for q in range(pieces):
            for turn in range(2):
                near_copy(g, q, turn).start()

    def relay(g, q):
        for turn in range(2):
            near_wait(g, q, turn)
            if q < late[1]:
                far_copy(g, q, turn).start()
                continue
            pl.when(g < last[0])(far_copy(g, q, turn).start)
            if q == late[1]:
                final = g == last[0]
                pl.when(final & (chip != chips - 2))(late_copy(turn, pl.ds(0, width)).start)
                pl.when(final & (chip == chips - 2))(late_copy(turn, rear).start)

    def dot(a, b):
        return jnp.dot(a, b, preferred_element_type=jnp.float32)

    def prepare():
        rows = groups * width
        raw_copy.wait()
        mix_copy.wait()
        bias_copy.wait()
        spread[...] = jnp.zeros_like(spread)
        for page in range(spread.shape[0]):
            size = min(LANES, tap_count - page * LANES)
            spread[page, :, pl.ds(0, size)] = raw[:, pl.ds(page * LANES, size)].astype(jnp.float32)
        fit = LANES // strip_rows
        lane = lax.broadcasted_iota(jnp.int32, (rows, LANES), 1)
        for first in range(0, width, fit):
            for s in range(segments):
                line = jnp.zeros((rows, LANES), jnp.float32)
                for n in range(fit):
                    source = pl.ds(first + n, rows, stride=width)
                    part_line = spread[s * strip_rows // LANES, source, :]
                    shift = (n * strip_rows - s * strip_rows) % LANES
                    part_line = pltpu.roll(part_line, shift, 1) if shift else part_line
                    line = jnp.where(lane // strip_rows == n, part_line, line)
                taps[s, :, :, pl.ds(first * strip_rows, LANES)] = line.reshape(groups, width, LANES)
        shape = (rows, rows * strip_rows)
        pick = lax.broadcasted_iota(jnp.int32, shape, 1) // strip_rows == lax.broadcasted_iota(jnp.int32, shape, 0)
        expanded = lax.dot_general(
            raw_mix[...],
            pick.astype(raw_mix.dtype),
            (((0,), (0,)), ((), ())),
            preferred_element_type=jnp.float32,
        )
        mixes[...] = expanded.reshape(mixes.shape)

    def build(g):
        slot = lax.rem(g, 2)
        shape = (strip_rows, LANES)
        row = lax.broadcasted_iota(jnp.int32, shape, 0)
        lane = lax.rem(lax.broadcasted_iota(jnp.int32, shape, 1), strip_rows)
        inside = lane >= row
        same = lane == row
        for o in range(width):
            rows = pl.ds(o * strip_rows, strip_rows)
            source = pl.ds(o, 1)
            for first in range(0, block, LANES):
                before = jnp.zeros(shape, jnp.float32)
                for s in range(segments):
                    line = jnp.broadcast_to(taps[s, g, source, pl.ds(first, LANES)], shape)
                    here = pltpu.roll(line, 0, 1, stride=1, stride_axis=0)
                    weights[lax.rem(g, 3), s, rows, pl.ds(first, LANES)] = jnp.where(inside, here, before).astype(jnp.bfloat16)
                    before = pltpu.roll(line, LANES - strip_rows, 1, stride=1, stride_axis=0)
            for first in range(0, groups * block, LANES):
                line = jnp.broadcast_to(mixes[g, source, pl.ds(first, LANES)], shape)
                mixer[rows, pl.ds(first, LANES)] = jnp.where(same, line, 0.0).astype(jnp.bfloat16)

    def wide(ref, first, count):
        return jnp.concatenate([ref[first + k].reshape(block, piece) for k in range(count)], axis=1)

    def inner(g):
        slot = lax.rem(g, 2)
        for n in range(pairs):
            for b in range(CORES):
                value = None
                for t in range(CORES):
                    term = dot(weights[lax.rem(g, 3), t - b + CORES], wide(own.at[t, g], n * PAIR, PAIR))
                    value = term if value is None else value + term
                for i in range(groups):
                    value += dot(mixer[:, pl.ds(i * block, block)], wide(own.at[b, i], n * PAIR, PAIR))
                total[slot, b, :, pl.ds(n * span, span)] = value

    def outer(g, first, count, tail=False):
        slot = lax.rem(g, 2)
        cols = pl.ds(first * piece, count * piece)
        for q in range(first, first + count):
            for turn in range(2):
                if not tail or q != late[1]:
                    far_copy(g, q, turn).wait_recv()
                    continue
                pl.when(chip > 0)(far_copy(g, q, turn).wait_recv)

                @pl.when(chip == 0)
                def _():
                    late_copy(turn, rear).wait_recv()
                    wrap_arrived(turn)

        for b in range(CORES):
            value = total[slot, b, :, cols]
            for role in range(2):
                for t in range(CORES):
                    s = t + (2 * CORES if role else 0) - b
                    if 0 <= s < segments:
                        value += dot(weights[lax.rem(g, 3), s], wide(halo.at[role, t, g], first, count))
            for o in range(width):
                x = value[o * strip_rows : (o + 1) * strip_rows] + bias[g * width + o]
                staged[b, g, o, :, cols] = jax.nn.gelu(x).astype(jnp.bfloat16)
        place = pl.ds(pl.multiple_of(core * part + first * piece, piece), count * piece)
        pltpu.make_async_copy(staged.at[core, g, :, :, cols], out.at[g, :, :, place], out_sem).start()
        pltpu.make_async_remote_copy(
            src_ref=staged.at[1 - core, g, :, :, cols],
            dst_ref=out.at[g, :, :, place],
            send_sem=out_send,
            recv_sem=out_recv,
            device_id=(peer,),
            device_id_type=MESH,
        ).start()

    load(0)
    load(groups - 1)
    barrier = pltpu.get_barrier_semaphore()
    def signal(sem, devices):
        for device in devices:
            pl.semaphore_signal(sem, inc=1, device_id=(device,), device_id_type=MESH)

    close = (*near, peer)
    above = (up_chip * CORES, up_chip * CORES + 1)
    below = (down_chip * CORES, down_chip * CORES + 1)
    first_chips, last_chips = chip < 2, chip >= chips - 2
    signal(barrier, close)
    pl.when(jnp.logical_not(last_chips))(lambda: signal(barrier, above))
    pl.when(first_chips)(lambda: signal(barrier, below))
    raw_copy = pltpu.make_async_copy(row_kernel, raw, param_sem.at[0])
    mix_copy = pltpu.make_async_copy(mix_weight, raw_mix, param_sem.at[1])
    bias_copy = pltpu.make_async_copy(channel_bias, bias, param_sem.at[2])
    for g in range(1, groups - 1):
        load(g)
    raw_copy.start()
    mix_copy.start()
    bias_copy.start()
    inner_chip = jnp.minimum(lax.div(chip, 2), 1)
    final_chip = lax.div(chip + 2, chips)
    pl.semaphore_wait(barrier, len(close) + len(below) * inner_chip + len(above) * final_chip)
    pl.when(jnp.logical_not(first_chips))(lambda: signal(ready, below))
    pl.when(last_chips)(lambda: signal(ready_wrap, above))

    def wait_above():
        @pl.when(jnp.logical_not(last_chips))
        def _():
            pl.semaphore_wait(ready, len(above))

    def hop():
        for turn in range(2):
            hop_copy(turn).start()

    loaded(0)
    send_near(0)
    loaded(groups - 1)
    pl.when(odd == 1)(wait_above)
    pl.when(chip > 0)(hop)

    @pl.when(chip == chips - 1)
    def _():
        for turn in range(2):
            wrap_copy(turn).start()

    for g in range(1, AHEAD):
        loaded(g)
        send_near(g)
    for g in range(AHEAD, groups - 1):
        loaded(g)
    for g in range(groups):
        swap(g).start()
    prepare()
    pltpu.make_async_remote_copy(
        src_ref=other,
        dst_ref=own.at[1 - core],
        send_sem=own_send,
        recv_sem=own_recv,
        device_id=(peer,),
        device_id_type=MESH,
    ).wait_recv()

    pl.when(odd == 0)(wait_above)

    @pl.when(chip == 1)
    def _():
        pl.semaphore_wait(ready_wrap, len(below))

    def step(g, carry):
        @pl.when((g == 1) & (chip == 0))
        def _():
            pl.semaphore_wait(ready_wrap, len(below))
            hop()

        @pl.when(g == groups - 1)
        def _():
            for turn in range(2):
                hop_copy(turn).wait_recv()
                hop_forward(turn).start()

            @pl.when(chip == 1)
            def _():
                for turn in range(2):
                    wrap_copy(turn).wait_recv()
                    wrap_forward(turn).start()

        @pl.when(g + AHEAD < groups)
        def _():
            send_near(g + AHEAD)

        relay(g, 0)

        @pl.when(g == 0)
        def _():
            build(g)
            inner(g)

        @pl.when(g + 1 < groups)
        def _():
            build(g + 1)

        relay(g, 1)

        @pl.when(g > 0)
        def _():
            outer(g - 1, PAIR, PAIR)

        relay(g, 2)

        @pl.when(g + 1 < groups)
        def _():
            inner(g + 1)

        relay(g, 3)
        outer(g, 0, PAIR)
        return carry

    lax.fori_loop(0, groups, step, 0)
    for q in reversed(range(PAIR, pieces)):
        outer(groups - 1, q, 1, tail=True)

    def sent(ref, sem):
        pltpu.make_async_remote_copy(
            src_ref=ref,
            dst_ref=ref,
            send_sem=sem,
            recv_sem=out_recv,
            device_id=(peer,),
            device_id_type=MESH,
        ).wait_send()

    sent(other, own_send)
    sent(features, near_send)
    for g in range(groups - 1):
        sent(halo.at[0, :, g], far_send.at[g])
    sent(halo.at[0, :, last[0], pl.ds(0, last[1])], far_send.at[last[0]])
    pl.when(chip != chips - 2)(lambda: sent(stage, late_send))
    pl.when(chip == chips - 2)(lambda: sent(stage_wrap, late_send))
    pl.when(chip == chips - 1)(lambda: sent(stage_wrap, wrap_send))
    pl.when(chip == 1)(lambda: sent(stage_wrap, wrap_pass))
    sent(stage, hop_send)
    pltpu.make_async_copy(staged.at[core], out.at[:, :, :, half(core)], out_sem).wait()
    swapped = pltpu.make_async_remote_copy(
        src_ref=staged.at[1 - core],
        dst_ref=out.at[:, :, :, half(1 - core)],
        send_sem=out_send,
        recv_sem=out_recv,
        device_id=(peer,),
        device_id_type=MESH,
    )
    swapped.wait_send()
    swapped.wait_recv()


def fixed(array):
    return pltpu.with_memory_space_constraint(array, pltpu.HBM)


def local(chips, features, row_kernel, mix_weight, channel_bias):
    channels, strip_rows, columns = features.shape
    groups, width, _, tap_count = row_kernel.shape
    assert tap_count - 1 == 2 * CORES * strip_rows and LANES % strip_rows == 0
    segments = 2 * CORES + 1
    part = columns // CORES
    block = width * strip_rows
    pieces = part // LANES
    assert pieces == 4
    dma = pltpu.SemaphoreType.DMA
    bf16 = features.dtype
    shape = (groups, width, strip_rows, columns)
    buffer = (groups, pieces, width, strip_rows, LANES)
    anywhere = pl.BlockSpec(memory_space=pl.ANY)
    out = pl.pallas_call(
        functools.partial(kernel, chips),
        name="layer",
        out_shape=jax.ShapeDtypeStruct(shape, bf16),
        in_specs=[pl.BlockSpec(memory_space=pltpu.HBM)] * 4,
        out_specs=anywhere,
        scratch_shapes=[
            pltpu.VMEM((CORES, *buffer), bf16),
            pltpu.VMEM(buffer, bf16),
            pltpu.VMEM((2, CORES, *buffer), bf16),
            pltpu.VMEM((channels * width, tap_count), row_kernel.dtype),
            pltpu.VMEM((channels, channels), mix_weight.dtype),
            pltpu.SMEM((channels,), channel_bias.dtype),
            pltpu.VMEM((pl.cdiv(tap_count, LANES), channels * width, LANES), jnp.float32),
            pltpu.VMEM((segments, groups, width, block), jnp.float32),
            pltpu.VMEM((groups, width, channels * strip_rows), jnp.float32),
            pltpu.VMEM((3, segments, block, block), bf16),
            pltpu.VMEM((block, channels * strip_rows), bf16),
            pltpu.VMEM((2, CORES, block, part), jnp.float32),
            pltpu.VMEM((CORES, groups, width, strip_rows, part), bf16),
            pltpu.VMEM((2, width, strip_rows, LANES), bf16),
            pltpu.VMEM((2, width // 2, strip_rows, LANES), bf16),
            dma((groups,)),
            dma((3,)),
            dma,
            dma,
            dma,
            dma((groups, pieces, CORES)),
            dma((groups,)),
            dma((groups, pieces, CORES)),
            dma,
            dma,
            dma,
            dma,
            dma((2,)),
            pltpu.SemaphoreType.REGULAR,
            pltpu.SemaphoreType.REGULAR,
            dma,
            dma,
            dma((2,)),
            dma,
            dma((2,)),
        ],
        compiler_params=pltpu.CompilerParams(
            collective_id=0, has_side_effects=True, vmem_limit_bytes=48 * 1024 * 1024
        ),
    )(
        features.reshape(shape),
        fixed(row_kernel.reshape(channels * width, tap_count)),
        fixed(mix_weight),
        fixed(channel_bias),
    )
    return out.reshape(features.shape)


def solution(mesh):
    chips = mesh.shape["strip"] // CORES
    assert chips % 2 == 0 and chips >= 4
    return jax.shard_map(
        functools.partial(local, chips),
        mesh=mesh,
        in_specs=(P(None, "strip", None), P(), P(), P()),
        out_specs=P(None, "strip", None),
        check_vma=False,
    )
```

```python
import functools

import jax
import jax.numpy as jnp
from jax import lax
from jax.experimental import pallas as pl
from jax.experimental.pallas import tpu as pltpu
from jax.sharding import PartitionSpec as P

MESH = pl.DeviceIdType.MESH
CORES = 2
LANES = 128
PAIR = 2
AHEAD = 2


def kernel(
    chips,
    features,
    row_kernel,
    mix_weight,
    channel_bias,
    out,
    own,
    other,
    halo,
    raw,
    raw_mix,
    bias,
    spread,
    taps,
    mixes,
    weights,
    mixer,
    total,
    staged,
    stage,
    stage_wrap,
    load_sem,
    param_sem,
    own_send,
    own_recv,
    near_send,
    near_recv,
    far_send,
    far_recv,
    out_sem,
    out_send,
    out_recv,
    hop_send,
    hop_recv,
    ready,
    ready_wrap,
    late_send,
    wrap_send,
    wrap_recv,
    wrap_pass,
    wrap_done,
):
    groups, width, strip_rows, columns = features.shape
    _, _, _, pieces, _, _, piece = halo.shape
    segments = weights.shape[1]
    tap_count = row_kernel.shape[1]
    part = columns // CORES
    block = width * strip_rows
    pairs = pieces // PAIR
    span = PAIR * piece

    me = lax.axis_index("strip")
    chip, core = lax.div(me, CORES), lax.rem(me, CORES)
    odd = lax.rem(chip, 2)
    near_chip = chip + 1 - 2 * odd
    far_chip = lax.rem(chip + 2 + odd * (chips - 4), chips)
    back_chip = lax.rem(chip + (chips - 2) - odd * (chips - 4), chips)
    peer = chip * CORES + 1 - core
    far = far_chip * CORES + core
    near = (near_chip * CORES + core, near_chip * CORES + 1 - core)
    back = (back_chip * CORES + core, back_chip * CORES + 1 - core)
    up_chip = lax.rem(chip + 2, chips)
    down_chip = lax.rem(chip + chips - 2, chips)
    last = (groups - 1, pieces - 1)
    late = (groups - 1, pieces - 2)
    front = pl.ds(0, width // 2)
    rear = pl.ds(width // 2, width // 2)

    def half(which):
        return pl.ds(pl.multiple_of(which * part, part), part)

    def load(g):
        for mine, which in ((own.at[core], core), (other, 1 - core)):
            for q in range(pieces):
                place = pl.ds(pl.multiple_of(which * part + q * piece, piece), piece)
                pltpu.make_async_copy(features.at[g, :, :, place], mine.at[g, q], load_sem.at[g]).start()

    def loaded(g):
        pltpu.make_async_copy(features.at[g], features.at[g], load_sem.at[g]).wait()

    def swap(g):
        return pltpu.make_async_remote_copy(
            src_ref=other.at[g],
            dst_ref=own.at[core, g],
            send_sem=own_send,
            recv_sem=own_recv,
            device_id=(peer,),
            device_id_type=MESH,
        )

    def near_copy(g, q, turn):
        return pltpu.make_async_remote_copy(
            src_ref=other.at[g, q] if turn else own.at[core, g, q],
            dst_ref=halo.at[odd, core, g, q],
            send_sem=near_send,
            recv_sem=near_recv.at[g, q, turn],
            device_id=(near[turn],),
            device_id_type=MESH,
        )

    def far_copy(g, q, turn):
        t = 1 - core if turn else core
        return pltpu.make_async_remote_copy(
            src_ref=halo.at[1 - odd, t, g, q],
            dst_ref=halo.at[odd, t, g, q],
            send_sem=far_send.at[g],
            recv_sem=far_recv.at[g, q, turn],
            device_id=(far,),
            device_id_type=MESH,
        )

    def near_wait(g, q, turn):
        region = halo.at[1 - odd, 1 - core if turn else core, g, q]
        pltpu.make_async_remote_copy(
            src_ref=region,
            dst_ref=region,
            send_sem=near_send,
            recv_sem=near_recv.at[g, q, turn],
            device_id=(far,),
            device_id_type=MESH,
        ).wait_recv()

    def hop_copy(turn):
        return pltpu.make_async_remote_copy(
            src_ref=other.at[last] if turn else own.at[core, *last],
            dst_ref=stage.at[turn],
            send_sem=hop_send,
            recv_sem=hop_recv.at[turn],
            device_id=(back[turn],),
            device_id_type=MESH,
        )

    def hop_forward(turn):
        return pltpu.make_async_remote_copy(
            src_ref=stage.at[turn],
            dst_ref=halo.at[1 - odd, 1 - core if turn else core, *last],
            send_sem=far_send.at[last[0]],
            recv_sem=far_recv.at[*last, turn],
            device_id=(near[0],),
            device_id_type=MESH,
        )

    def late_copy(turn, part_rows):
        t = 1 - core if turn else core
        return pltpu.make_async_remote_copy(
            src_ref=halo.at[1 - odd, t, *late, part_rows],
            dst_ref=halo.at[odd, t, *late, part_rows],
            send_sem=late_send,
            recv_sem=far_recv.at[*late, turn],
            device_id=(far,),
            device_id_type=MESH,
        )

    def wrap_copy(turn):
        return pltpu.make_async_remote_copy(
            src_ref=other.at[*late, front] if turn else own.at[core, *late, front],
            dst_ref=stage_wrap.at[turn],
            send_sem=wrap_send,
            recv_sem=wrap_recv.at[turn],
            device_id=(back[turn],),
            device_id_type=MESH,
        )

    def wrap_forward(turn):
        return pltpu.make_async_remote_copy(
            src_ref=stage_wrap.at[turn],
            dst_ref=halo.at[1 - odd, 1 - core if turn else core, *late, front],
            send_sem=wrap_pass,
            recv_sem=wrap_done.at[turn],
            device_id=(near[0],),
            device_id_type=MESH,
        )

    def wrap_arrived(turn):
        region = halo.at[odd, 1 - core if turn else core, *late, front]
        pltpu.make_async_remote_copy(
            src_ref=region,
            dst_ref=region,
            send_sem=wrap_pass,
            recv_sem=wrap_done.at[turn],
            device_id=(near[0],),
            device_id_type=MESH,
        ).wait_recv()

    def send_near(g):
        for q in range(pieces):
            for turn in range(2):
                near_copy(g, q, turn).start()

    def relay(g, q):
        for turn in range(2):
            near_wait(g, q, turn)
            if q < late[1]:
                far_copy(g, q, turn).start()
                continue
            pl.when(g < last[0])(far_copy(g, q, turn).start)
            if q == late[1]:
                final = g == last[0]
                pl.when(final & (chip != chips - 2))(late_copy(turn, pl.ds(0, width)).start)
                pl.when(final & (chip == chips - 2))(late_copy(turn, rear).start)

    def dot(a, b):
        return jnp.dot(a, b, preferred_element_type=jnp.float32)

    def prepare():
        rows = groups * width
        raw_copy.wait()
        mix_copy.wait()
        bias_copy.wait()
        spread[...] = jnp.zeros_like(spread)
        for page in range(spread.shape[0]):
            size = min(LANES, tap_count - page * LANES)
            spread[page, :, pl.ds(0, size)] = raw[:, pl.ds(page * LANES, size)].astype(jnp.float32)
        fit = LANES // strip_rows
        lane = lax.broadcasted_iota(jnp.int32, (rows, LANES), 1)
        for first in range(0, width, fit):
            for s in range(segments):
                line = jnp.zeros((rows, LANES), jnp.float32)
                for n in range(fit):
                    source = pl.ds(first + n, rows, stride=width)
                    part_line = spread[s * strip_rows // LANES, source, :]
                    shift = (n * strip_rows - s * strip_rows) % LANES
                    part_line = pltpu.roll(part_line, shift, 1) if shift else part_line
                    line = jnp.where(lane // strip_rows == n, part_line, line)
                taps[s, :, :, pl.ds(first * strip_rows, LANES)] = line.reshape(groups, width, LANES)
        shape = (rows, rows * strip_rows)
        pick = lax.broadcasted_iota(jnp.int32, shape, 1) // strip_rows == lax.broadcasted_iota(jnp.int32, shape, 0)
        expanded = lax.dot_general(
            raw_mix[...],
            pick.astype(raw_mix.dtype),
            (((0,), (0,)), ((), ())),
            preferred_element_type=jnp.float32,
        )
        mixes[...] = expanded.reshape(mixes.shape)

    def build(g):
        slot = lax.rem(g, 2)
        shape = (strip_rows, LANES)
        row = lax.broadcasted_iota(jnp.int32, shape, 0)
        lane = lax.rem(lax.broadcasted_iota(jnp.int32, shape, 1), strip_rows)
        inside = lane >= row
        same = lane == row
        for o in range(width):
            rows = pl.ds(o * strip_rows, strip_rows)
            source = pl.ds(o, 1)
            for first in range(0, block, LANES):
                before = jnp.zeros(shape, jnp.float32)
                for s in range(segments):
                    line = jnp.broadcast_to(taps[s, g, source, pl.ds(first, LANES)], shape)
                    here = pltpu.roll(line, 0, 1, stride=1, stride_axis=0)
                    weights[lax.rem(g, 3), s, rows, pl.ds(first, LANES)] = jnp.where(inside, here, before).astype(jnp.bfloat16)
                    before = pltpu.roll(line, LANES - strip_rows, 1, stride=1, stride_axis=0)
            for first in range(0, groups * block, LANES):
                line = jnp.broadcast_to(mixes[g, source, pl.ds(first, LANES)], shape)
                mixer[rows, pl.ds(first, LANES)] = jnp.where(same, line, 0.0).astype(jnp.bfloat16)

    def wide(ref, first, count):
        return jnp.concatenate([ref[first + k].reshape(block, piece) for k in range(count)], axis=1)

    def inner(g):
        slot = lax.rem(g, 2)
        for n in range(pairs):
            for b in range(CORES):
                value = None
                for t in range(CORES):
                    term = dot(weights[lax.rem(g, 3), t - b + CORES], wide(own.at[t, g], n * PAIR, PAIR))
                    value = term if value is None else value + term
                for i in range(groups):
                    value += dot(mixer[:, pl.ds(i * block, block)], wide(own.at[b, i], n * PAIR, PAIR))
                total[slot, b, :, pl.ds(n * span, span)] = value

    def outer(g, first, count, tail=False):
        slot = lax.rem(g, 2)
        cols = pl.ds(first * piece, count * piece)
        for q in range(first, first + count):
            for turn in range(2):
                if not tail or q != late[1]:
                    far_copy(g, q, turn).wait_recv()
                    continue
                pl.when(chip > 0)(far_copy(g, q, turn).wait_recv)

                @pl.when(chip == 0)
                def _():
                    late_copy(turn, rear).wait_recv()
                    wrap_arrived(turn)

        place = pl.ds(pl.multiple_of(core * part + first * piece, piece), count * piece)

        def finish(b):
            value = total[slot, b, :, cols]
            for role, t, s in ((0, b, 0), (b, 1 - b, 1 + b * (segments - 3)), (1, b, segments - 1)):
                value += dot(weights[lax.rem(g, 3), s], wide(halo.at[role, t, g], first, count))
            for o in range(width):
                x = value[o * strip_rows : (o + 1) * strip_rows] + bias[g * width + o]
                staged[b, g, o, :, cols] = jax.nn.gelu(x).astype(jnp.bfloat16)

        finish(1 - core)
        pltpu.make_async_remote_copy(
            src_ref=staged.at[1 - core, g, :, :, cols],
            dst_ref=out.at[g, :, :, place],
            send_sem=out_send,
            recv_sem=out_recv,
            device_id=(peer,),
            device_id_type=MESH,
        ).start()
        finish(core)
        pltpu.make_async_copy(staged.at[core, g, :, :, cols], out.at[g, :, :, place], out_sem).start()

    load(0)
    load(groups - 1)
    barrier = pltpu.get_barrier_semaphore()
    def signal(sem, devices):
        for device in devices:
            pl.semaphore_signal(sem, inc=1, device_id=(device,), device_id_type=MESH)

    close = (*near, peer)
    above = (up_chip * CORES, up_chip * CORES + 1)
    below = (down_chip * CORES, down_chip * CORES + 1)
    first_chips, last_chips = chip < 2, chip >= chips - 2
    signal(barrier, close)
    pl.when(jnp.logical_not(last_chips))(lambda: signal(barrier, above))
    pl.when(first_chips)(lambda: signal(barrier, below))
    raw_copy = pltpu.make_async_copy(row_kernel, raw, param_sem.at[0])
    mix_copy = pltpu.make_async_copy(mix_weight, raw_mix, param_sem.at[1])
    bias_copy = pltpu.make_async_copy(channel_bias, bias, param_sem.at[2])
    for g in range(1, groups - 1):
        load(g)
    raw_copy.start()
    mix_copy.start()
    bias_copy.start()
    inner_chip = jnp.minimum(lax.div(chip, 2), 1)
    final_chip = lax.div(chip + 2, chips)
    pl.semaphore_wait(barrier, len(close) + len(below) * inner_chip + len(above) * final_chip)
    pl.when(jnp.logical_not(first_chips))(lambda: signal(ready, below))
    pl.when(last_chips)(lambda: signal(ready_wrap, above))

    def wait_above():
        @pl.when(jnp.logical_not(last_chips))
        def _():
            pl.semaphore_wait(ready, len(above))

    def hop():
        for turn in range(2):
            hop_copy(turn).start()

    loaded(0)
    send_near(0)
    loaded(groups - 1)
    pl.when(odd == 1)(wait_above)
    pl.when(chip > 0)(hop)

    @pl.when(chip == chips - 1)
    def _():
        for turn in range(2):
            wrap_copy(turn).start()

    for g in range(1, AHEAD):
        loaded(g)
        send_near(g)
    for g in range(AHEAD, groups - 1):
        loaded(g)
    for g in range(groups):
        swap(g).start()
    prepare()
    pltpu.make_async_remote_copy(
        src_ref=other,
        dst_ref=own.at[1 - core],
        send_sem=own_send,
        recv_sem=own_recv,
        device_id=(peer,),
        device_id_type=MESH,
    ).wait_recv()

    pl.when(odd == 0)(wait_above)

    @pl.when(chip == 1)
    def _():
        pl.semaphore_wait(ready_wrap, len(below))

    def step(g, carry):
        @pl.when((g == 1) & (chip == 0))
        def _():
            pl.semaphore_wait(ready_wrap, len(below))
            hop()

        @pl.when(g + AHEAD < groups)
        def _():
            send_near(g + AHEAD)

        relay(g, 0)

        @pl.when(g == 0)
        def _():
            build(g)
            inner(g)

        @pl.when(g + 1 < groups)
        def _():
            build(g + 1)

        relay(g, 1)

        @pl.when(g > 0)
        def _():
            outer(g - 1, PAIR, PAIR)

        relay(g, 2)

        @pl.when(g == groups - 1)
        def _():
            for turn in range(2):
                hop_copy(turn).wait_recv()
                hop_forward(turn).start()

            @pl.when(chip == 1)
            def _():
                for turn in range(2):
                    wrap_copy(turn).wait_recv()
                    wrap_forward(turn).start()

        @pl.when(g + 1 < groups)
        def _():
            inner(g + 1)

        relay(g, 3)
        outer(g, 0, PAIR)
        return carry

    lax.fori_loop(0, groups, step, 0)
    for q in reversed(range(PAIR, pieces)):
        outer(groups - 1, q, 1, tail=True)

    def sent(ref, sem):
        pltpu.make_async_remote_copy(
            src_ref=ref,
            dst_ref=ref,
            send_sem=sem,
            recv_sem=out_recv,
            device_id=(peer,),
            device_id_type=MESH,
        ).wait_send()

    sent(other, own_send)
    sent(features, near_send)
    for g in range(groups - 1):
        sent(halo.at[0, :, g], far_send.at[g])
    sent(halo.at[0, :, last[0], pl.ds(0, last[1])], far_send.at[last[0]])
    pl.when(chip != chips - 2)(lambda: sent(stage, late_send))
    pl.when(chip == chips - 2)(lambda: sent(stage_wrap, late_send))
    pl.when(chip == chips - 1)(lambda: sent(stage_wrap, wrap_send))
    pl.when(chip == 1)(lambda: sent(stage_wrap, wrap_pass))
    sent(stage, hop_send)
    pltpu.make_async_copy(staged.at[core], out.at[:, :, :, half(core)], out_sem).wait()
    swapped = pltpu.make_async_remote_copy(
        src_ref=staged.at[1 - core],
        dst_ref=out.at[:, :, :, half(1 - core)],
        send_sem=out_send,
        recv_sem=out_recv,
        device_id=(peer,),
        device_id_type=MESH,
    )
    swapped.wait_send()
    swapped.wait_recv()


def fixed(array):
    return pltpu.with_memory_space_constraint(array, pltpu.HBM)


def local(chips, features, row_kernel, mix_weight, channel_bias):
    channels, strip_rows, columns = features.shape
    groups, width, _, tap_count = row_kernel.shape
    assert tap_count - 1 == 2 * CORES * strip_rows and LANES % strip_rows == 0
    segments = 2 * CORES + 1
    part = columns // CORES
    block = width * strip_rows
    pieces = part // LANES
    assert pieces == 4
    dma = pltpu.SemaphoreType.DMA
    bf16 = features.dtype
    shape = (groups, width, strip_rows, columns)
    buffer = (groups, pieces, width, strip_rows, LANES)
    anywhere = pl.BlockSpec(memory_space=pl.ANY)
    out = pl.pallas_call(
        functools.partial(kernel, chips),
        name="layer",
        out_shape=jax.ShapeDtypeStruct(shape, bf16),
        in_specs=[pl.BlockSpec(memory_space=pltpu.HBM)] * 4,
        out_specs=anywhere,
        scratch_shapes=[
            pltpu.VMEM((CORES, *buffer), bf16),
            pltpu.VMEM(buffer, bf16),
            pltpu.VMEM((2, CORES, *buffer), bf16),
            pltpu.VMEM((channels * width, tap_count), row_kernel.dtype),
            pltpu.VMEM((channels, channels), mix_weight.dtype),
            pltpu.SMEM((channels,), channel_bias.dtype),
            pltpu.VMEM((pl.cdiv(tap_count, LANES), channels * width, LANES), jnp.float32),
            pltpu.VMEM((segments, groups, width, block), jnp.float32),
            pltpu.VMEM((groups, width, channels * strip_rows), jnp.float32),
            pltpu.VMEM((3, segments, block, block), bf16),
            pltpu.VMEM((block, channels * strip_rows), bf16),
            pltpu.VMEM((2, CORES, block, part), jnp.float32),
            pltpu.VMEM((CORES, groups, width, strip_rows, part), bf16),
            pltpu.VMEM((2, width, strip_rows, LANES), bf16),
            pltpu.VMEM((2, width // 2, strip_rows, LANES), bf16),
            dma((groups,)),
            dma((3,)),
            dma,
            dma,
            dma,
            dma((groups, pieces, CORES)),
            dma((groups,)),
            dma((groups, pieces, CORES)),
            dma,
            dma,
            dma,
            dma,
            dma((2,)),
            pltpu.SemaphoreType.REGULAR,
            pltpu.SemaphoreType.REGULAR,
            dma,
            dma,
            dma((2,)),
            dma,
            dma((2,)),
        ],
        compiler_params=pltpu.CompilerParams(
            collective_id=0, has_side_effects=True, vmem_limit_bytes=48 * 1024 * 1024
        ),
    )(
        features.reshape(shape),
        fixed(row_kernel.reshape(channels * width, tap_count)),
        fixed(mix_weight),
        fixed(channel_bias),
    )
    return out.reshape(features.shape)


def solution(mesh):
    chips = mesh.shape["strip"] // CORES
    assert chips % 2 == 0 and chips >= 4
    return jax.shard_map(
        functools.partial(local, chips),
        mesh=mesh,
        in_specs=(P(None, "strip", None), P(), P(), P()),
        out_specs=P(None, "strip", None),
        check_vma=False,
    )
```

```python
import functools

import jax
import jax.numpy as jnp
from jax import lax
from jax.experimental import pallas as pl
from jax.experimental.pallas import tpu as pltpu
from jax.sharding import PartitionSpec as P

MESH = pl.DeviceIdType.MESH
CORES = 2
LANES = 128
PAIR = 2
AHEAD = 2


def kernel(
    chips,
    features,
    row_kernel,
    mix_weight,
    channel_bias,
    out,
    own,
    other,
    halo,
    raw,
    raw_mix,
    bias,
    spread,
    taps,
    mixes,
    weights,
    mixer,
    total,
    staged,
    stage,
    stage_wrap,
    load_sem,
    param_sem,
    own_send,
    own_recv,
    near_send,
    near_recv,
    far_send,
    far_recv,
    out_sem,
    out_send,
    out_recv,
    hop_send,
    hop_recv,
    ready,
    ready_wrap,
    late_send,
    wrap_send,
    wrap_recv,
    wrap_pass,
    wrap_done,
):
    groups, width, strip_rows, columns = features.shape
    _, _, _, pieces, _, _, piece = halo.shape
    segments = weights.shape[1]
    tap_count = row_kernel.shape[1]
    part = columns // CORES
    block = width * strip_rows
    pairs = pieces // PAIR
    span = PAIR * piece

    me = lax.axis_index("strip")
    chip, core = lax.div(me, CORES), lax.rem(me, CORES)
    odd = lax.rem(chip, 2)
    near_chip = chip + 1 - 2 * odd
    far_chip = lax.rem(chip + 2 + odd * (chips - 4), chips)
    back_chip = lax.rem(chip + (chips - 2) - odd * (chips - 4), chips)
    peer = chip * CORES + 1 - core
    far = far_chip * CORES + core
    near = (near_chip * CORES + core, near_chip * CORES + 1 - core)
    back = (back_chip * CORES + core, back_chip * CORES + 1 - core)
    up_chip = lax.rem(chip + 2, chips)
    down_chip = lax.rem(chip + chips - 2, chips)
    last = (groups - 1, pieces - 1)
    late = (groups - 1, pieces - 2)
    front = pl.ds(0, width // 2)
    rear = pl.ds(width // 2, width // 2)

    def half(which):
        return pl.ds(pl.multiple_of(which * part, part), part)

    def load(g):
        for mine, which in ((own.at[core], core), (other, 1 - core)):
            for q in range(pieces):
                place = pl.ds(pl.multiple_of(which * part + q * piece, piece), piece)
                pltpu.make_async_copy(features.at[g, :, :, place], mine.at[g, q], load_sem.at[g]).start()

    def loaded(g):
        pltpu.make_async_copy(features.at[g], features.at[g], load_sem.at[g]).wait()

    def swap(g):
        return pltpu.make_async_remote_copy(
            src_ref=other.at[g],
            dst_ref=own.at[core, g],
            send_sem=own_send,
            recv_sem=own_recv,
            device_id=(peer,),
            device_id_type=MESH,
        )

    def near_copy(g, q, turn):
        return pltpu.make_async_remote_copy(
            src_ref=other.at[g, q] if turn else own.at[core, g, q],
            dst_ref=halo.at[odd, core, g, q],
            send_sem=near_send,
            recv_sem=near_recv.at[g, q, turn],
            device_id=(near[turn],),
            device_id_type=MESH,
        )

    def far_copy(g, q, turn):
        t = 1 - core if turn else core
        return pltpu.make_async_remote_copy(
            src_ref=halo.at[1 - odd, t, g, q],
            dst_ref=halo.at[odd, t, g, q],
            send_sem=far_send.at[g],
            recv_sem=far_recv.at[g, q, turn],
            device_id=(far,),
            device_id_type=MESH,
        )

    def near_wait(g, q, turn):
        region = halo.at[1 - odd, 1 - core if turn else core, g, q]
        pltpu.make_async_remote_copy(
            src_ref=region,
            dst_ref=region,
            send_sem=near_send,
            recv_sem=near_recv.at[g, q, turn],
            device_id=(far,),
            device_id_type=MESH,
        ).wait_recv()

    def hop_copy(turn):
        return pltpu.make_async_remote_copy(
            src_ref=other.at[last] if turn else own.at[core, *last],
            dst_ref=stage.at[turn],
            send_sem=hop_send,
            recv_sem=hop_recv.at[turn],
            device_id=(back[turn],),
            device_id_type=MESH,
        )

    def hop_forward(turn):
        return pltpu.make_async_remote_copy(
            src_ref=stage.at[turn],
            dst_ref=halo.at[1 - odd, 1 - core if turn else core, *last],
            send_sem=far_send.at[last[0]],
            recv_sem=far_recv.at[*last, turn],
            device_id=(near[0],),
            device_id_type=MESH,
        )

    def late_copy(turn, part_rows):
        t = 1 - core if turn else core
        return pltpu.make_async_remote_copy(
            src_ref=halo.at[1 - odd, t, *late, part_rows],
            dst_ref=halo.at[odd, t, *late, part_rows],
            send_sem=late_send,
            recv_sem=far_recv.at[*late, turn],
            device_id=(far,),
            device_id_type=MESH,
        )

    def wrap_copy(turn):
        return pltpu.make_async_remote_copy(
            src_ref=other.at[*late, front] if turn else own.at[core, *late, front],
            dst_ref=stage_wrap.at[turn],
            send_sem=wrap_send,
            recv_sem=wrap_recv.at[turn],
            device_id=(back[turn],),
            device_id_type=MESH,
        )

    def wrap_forward(turn):
        return pltpu.make_async_remote_copy(
            src_ref=stage_wrap.at[turn],
            dst_ref=halo.at[1 - odd, 1 - core if turn else core, *late, front],
            send_sem=wrap_pass,
            recv_sem=wrap_done.at[turn],
            device_id=(near[0],),
            device_id_type=MESH,
        )

    def wrap_arrived(turn):
        region = halo.at[odd, 1 - core if turn else core, *late, front]
        pltpu.make_async_remote_copy(
            src_ref=region,
            dst_ref=region,
            send_sem=wrap_pass,
            recv_sem=wrap_done.at[turn],
            device_id=(near[0],),
            device_id_type=MESH,
        ).wait_recv()

    def send_near(g):
        for q in range(pieces):
            for turn in range(2):
                near_copy(g, q, turn).start()

    def relay(g, q):
        for turn in range(2):
            near_wait(g, q, turn)
            if q < late[1]:
                far_copy(g, q, turn).start()
                continue
            pl.when(g < last[0])(far_copy(g, q, turn).start)
            if q == late[1]:
                final = g == last[0]
                pl.when(final & (chip != chips - 2))(late_copy(turn, pl.ds(0, width)).start)
                pl.when(final & (chip == chips - 2))(late_copy(turn, rear).start)

    def dot(a, b):
        return jnp.dot(a, b, preferred_element_type=jnp.float32)

    def prepare():
        rows = groups * width
        raw_copy.wait()
        mix_copy.wait()
        bias_copy.wait()
        spread[...] = jnp.zeros_like(spread)
        for page in range(spread.shape[0]):
            size = min(LANES, tap_count - page * LANES)
            spread[page, :, pl.ds(0, size)] = raw[:, pl.ds(page * LANES, size)].astype(jnp.float32)
        fit = LANES // strip_rows
        lane = lax.broadcasted_iota(jnp.int32, (rows, LANES), 1)
        for first in range(0, width, fit):
            for s in range(segments):
                line = jnp.zeros((rows, LANES), jnp.float32)
                for n in range(fit):
                    source = pl.ds(first + n, rows, stride=width)
                    part_line = spread[s * strip_rows // LANES, source, :]
                    shift = (n * strip_rows - s * strip_rows) % LANES
                    part_line = pltpu.roll(part_line, shift, 1) if shift else part_line
                    line = jnp.where(lane // strip_rows == n, part_line, line)
                taps[s, :, :, pl.ds(first * strip_rows, LANES)] = line.reshape(groups, width, LANES)
        shape = (rows, rows * strip_rows)
        pick = lax.broadcasted_iota(jnp.int32, shape, 1) // strip_rows == lax.broadcasted_iota(jnp.int32, shape, 0)
        expanded = lax.dot_general(
            raw_mix[...],
            pick.astype(raw_mix.dtype),
            (((0,), (0,)), ((), ())),
            preferred_element_type=jnp.float32,
        )
        mixes[...] = expanded.reshape(mixes.shape)

    def build(g):
        slot = lax.rem(g, 2)
        shape = (strip_rows, LANES)
        row = lax.broadcasted_iota(jnp.int32, shape, 0)
        lane = lax.rem(lax.broadcasted_iota(jnp.int32, shape, 1), strip_rows)
        inside = lane >= row
        same = lane == row
        for o in range(width):
            rows = pl.ds(o * strip_rows, strip_rows)
            source = pl.ds(o, 1)
            for first in range(0, block, LANES):
                before = jnp.zeros(shape, jnp.float32)
                for s in range(segments):
                    line = jnp.broadcast_to(taps[s, g, source, pl.ds(first, LANES)], shape)
                    here = pltpu.roll(line, 0, 1, stride=1, stride_axis=0)
                    weights[lax.rem(g, 3), s, rows, pl.ds(first, LANES)] = jnp.where(inside, here, before).astype(jnp.bfloat16)
                    before = pltpu.roll(line, LANES - strip_rows, 1, stride=1, stride_axis=0)
            for first in range(0, groups * block, LANES):
                line = jnp.broadcast_to(mixes[g, source, pl.ds(first, LANES)], shape)
                mixer[rows, pl.ds(first, LANES)] = jnp.where(same, line, 0.0).astype(jnp.bfloat16)

    def wide(ref, first, count):
        return jnp.concatenate([ref[first + k].reshape(block, piece) for k in range(count)], axis=1)

    def inner(g):
        slot = lax.rem(g, 2)
        for n in range(pairs):
            for b in range(CORES):
                value = None
                for t in range(CORES):
                    term = dot(weights[lax.rem(g, 3), t - b + CORES], wide(own.at[t, g], n * PAIR, PAIR))
                    value = term if value is None else value + term
                for i in range(groups):
                    value += dot(mixer[:, pl.ds(i * block, block)], wide(own.at[b, i], n * PAIR, PAIR))
                total[slot, b, :, pl.ds(n * span, span)] = value

    def outer(g, first, count, tail=False):
        slot = lax.rem(g, 2)
        cols = pl.ds(first * piece, count * piece)
        for q in range(first, first + count):
            for turn in range(2):
                if not tail or q != late[1]:
                    far_copy(g, q, turn).wait_recv()
                    continue
                pl.when(chip > 0)(far_copy(g, q, turn).wait_recv)

                @pl.when(chip == 0)
                def _():
                    late_copy(turn, rear).wait_recv()
                    wrap_arrived(turn)

        for b in range(CORES):
            value = total[slot, b, :, cols]
            for role in range(2):
                for t in range(CORES):
                    s = t + (2 * CORES if role else 0) - b
                    if 0 <= s < segments:
                        value += dot(weights[lax.rem(g, 3), s], wide(halo.at[role, t, g], first, count))
            for o in range(width):
                x = value[o * strip_rows : (o + 1) * strip_rows] + bias[g * width + o]
                staged[b, g, o, :, cols] = jax.nn.gelu(x).astype(jnp.bfloat16)
        place = pl.ds(pl.multiple_of(core * part + first * piece, piece), count * piece)
        pltpu.make_async_copy(staged.at[core, g, :, :, cols], out.at[g, :, :, place], out_sem).start()
        pltpu.make_async_remote_copy(
            src_ref=staged.at[1 - core, g, :, :, cols],
            dst_ref=out.at[g, :, :, place],
            send_sem=out_send,
            recv_sem=out_recv,
            device_id=(peer,),
            device_id_type=MESH,
        ).start()

    load(0)
    load(groups - 1)
    barrier = pltpu.get_barrier_semaphore()
    def signal(sem, devices):
        for device in devices:
            pl.semaphore_signal(sem, inc=1, device_id=(device,), device_id_type=MESH)

    close = (*near, peer)
    above = (up_chip * CORES, up_chip * CORES + 1)
    below = (down_chip * CORES, down_chip * CORES + 1)
    first_chips, last_chips = chip < 2, chip >= chips - 2
    signal(barrier, close)
    pl.when(jnp.logical_not(last_chips))(lambda: signal(barrier, above))
    pl.when(first_chips)(lambda: signal(barrier, below))
    raw_copy = pltpu.make_async_copy(row_kernel, raw, param_sem.at[0])
    mix_copy = pltpu.make_async_copy(mix_weight, raw_mix, param_sem.at[1])
    bias_copy = pltpu.make_async_copy(channel_bias, bias, param_sem.at[2])
    for g in range(1, groups - 1):
        load(g)
    raw_copy.start()
    mix_copy.start()
    bias_copy.start()
    inner_chip = jnp.minimum(lax.div(chip, 2), 1)
    final_chip = lax.div(chip + 2, chips)
    pl.semaphore_wait(barrier, len(close) + len(below) * inner_chip + len(above) * final_chip)
    pl.when(jnp.logical_not(first_chips))(lambda: signal(ready, below))
    pl.when(last_chips)(lambda: signal(ready_wrap, above))

    def wait_above():
        @pl.when(jnp.logical_not(last_chips))
        def _():
            pl.semaphore_wait(ready, len(above))

    def hop():
        for turn in range(2):
            hop_copy(turn).start()

    loaded(0)
    send_near(0)
    loaded(groups - 1)
    pl.when(odd == 1)(wait_above)
    pl.when(chip > 0)(hop)

    @pl.when(chip == chips - 1)
    def _():
        for turn in range(2):
            wrap_copy(turn).start()

    for g in range(1, AHEAD):
        loaded(g)
        send_near(g)
    for g in range(AHEAD, groups - 1):
        loaded(g)
    for g in range(groups):
        swap(g).start()
    prepare()
    pltpu.make_async_remote_copy(
        src_ref=other,
        dst_ref=own.at[1 - core],
        send_sem=own_send,
        recv_sem=own_recv,
        device_id=(peer,),
        device_id_type=MESH,
    ).wait_recv()

    pl.when(odd == 0)(wait_above)

    @pl.when(chip == 1)
    def _():
        pl.semaphore_wait(ready_wrap, len(below))

    def step(g, carry):
        @pl.when((g == 1) & (chip == 0))
        def _():
            pl.semaphore_wait(ready_wrap, len(below))
            hop()

        @pl.when(g == groups - 1)
        def _():
            for turn in range(2):
                hop_copy(turn).wait_recv()
                hop_forward(turn).start()

            @pl.when(chip == 1)
            def _():
                for turn in range(2):
                    wrap_copy(turn).wait_recv()
                    wrap_forward(turn).start()

        relay(g, 0)

        @pl.when(g + AHEAD < groups)
        def _():
            send_near(g + AHEAD)

        @pl.when(g == 0)
        def _():
            build(g)
            inner(g)

        @pl.when(g + 1 < groups)
        def _():
            build(g + 1)

        relay(g, 1)

        @pl.when(g > 0)
        def _():
            outer(g - 1, PAIR, PAIR)

        relay(g, 2)

        @pl.when(g + 1 < groups)
        def _():
            inner(g + 1)

        relay(g, 3)
        outer(g, 0, PAIR)
        return carry

    lax.fori_loop(0, groups, step, 0)
    for q in reversed(range(PAIR, pieces)):
        outer(groups - 1, q, 1, tail=True)

    def sent(ref, sem):
        pltpu.make_async_remote_copy(
            src_ref=ref,
            dst_ref=ref,
            send_sem=sem,
            recv_sem=out_recv,
            device_id=(peer,),
            device_id_type=MESH,
        ).wait_send()

    sent(other, own_send)
    sent(features, near_send)
    for g in range(groups - 1):
        sent(halo.at[0, :, g], far_send.at[g])
    sent(halo.at[0, :, last[0], pl.ds(0, last[1])], far_send.at[last[0]])
    pl.when(chip != chips - 2)(lambda: sent(stage, late_send))
    pl.when(chip == chips - 2)(lambda: sent(stage_wrap, late_send))
    pl.when(chip == chips - 1)(lambda: sent(stage_wrap, wrap_send))
    pl.when(chip == 1)(lambda: sent(stage_wrap, wrap_pass))
    sent(stage, hop_send)
    pltpu.make_async_copy(staged.at[core], out.at[:, :, :, half(core)], out_sem).wait()
    swapped = pltpu.make_async_remote_copy(
        src_ref=staged.at[1 - core],
        dst_ref=out.at[:, :, :, half(1 - core)],
        send_sem=out_send,
        recv_sem=out_recv,
        device_id=(peer,),
        device_id_type=MESH,
    )
    swapped.wait_send()
    swapped.wait_recv()


def fixed(array):
    return pltpu.with_memory_space_constraint(array, pltpu.HBM)


def local(chips, features, row_kernel, mix_weight, channel_bias):
    channels, strip_rows, columns = features.shape
    groups, width, _, tap_count = row_kernel.shape
    assert tap_count - 1 == 2 * CORES * strip_rows and LANES % strip_rows == 0
    segments = 2 * CORES + 1
    part = columns // CORES
    block = width * strip_rows
    pieces = part // LANES
    assert pieces == 4
    dma = pltpu.SemaphoreType.DMA
    bf16 = features.dtype
    shape = (groups, width, strip_rows, columns)
    buffer = (groups, pieces, width, strip_rows, LANES)
    anywhere = pl.BlockSpec(memory_space=pl.ANY)
    out = pl.pallas_call(
        functools.partial(kernel, chips),
        name="layer",
        out_shape=jax.ShapeDtypeStruct(shape, bf16),
        in_specs=[pl.BlockSpec(memory_space=pltpu.HBM)] * 4,
        out_specs=anywhere,
        scratch_shapes=[
            pltpu.VMEM((CORES, *buffer), bf16),
            pltpu.VMEM(buffer, bf16),
            pltpu.VMEM((2, CORES, *buffer), bf16),
            pltpu.VMEM((channels * width, tap_count), row_kernel.dtype),
            pltpu.VMEM((channels, channels), mix_weight.dtype),
            pltpu.SMEM((channels,), channel_bias.dtype),
            pltpu.VMEM((pl.cdiv(tap_count, LANES), channels * width, LANES), jnp.float32),
            pltpu.VMEM((segments, groups, width, block), jnp.float32),
            pltpu.VMEM((groups, width, channels * strip_rows), jnp.float32),
            pltpu.VMEM((3, segments, block, block), bf16),
            pltpu.VMEM((block, channels * strip_rows), bf16),
            pltpu.VMEM((2, CORES, block, part), jnp.float32),
            pltpu.VMEM((CORES, groups, width, strip_rows, part), bf16),
            pltpu.VMEM((2, width, strip_rows, LANES), bf16),
            pltpu.VMEM((2, width // 2, strip_rows, LANES), bf16),
            dma((groups,)),
            dma((3,)),
            dma,
            dma,
            dma,
            dma((groups, pieces, CORES)),
            dma((groups,)),
            dma((groups, pieces, CORES)),
            dma,
            dma,
            dma,
            dma,
            dma((2,)),
            pltpu.SemaphoreType.REGULAR,
            pltpu.SemaphoreType.REGULAR,
            dma,
            dma,
            dma((2,)),
            dma,
            dma((2,)),
        ],
        compiler_params=pltpu.CompilerParams(
            collective_id=0, has_side_effects=True, vmem_limit_bytes=48 * 1024 * 1024
        ),
    )(
        features.reshape(shape),
        fixed(row_kernel.reshape(channels * width, tap_count)),
        fixed(mix_weight),
        fixed(channel_bias),
    )
    return out.reshape(features.shape)


def solution(mesh):
    chips = mesh.shape["strip"] // CORES
    assert chips % 2 == 0 and chips >= 4
    return jax.shard_map(
        functools.partial(local, chips),
        mesh=mesh,
        in_specs=(P(None, "strip", None), P(), P(), P()),
        out_specs=P(None, "strip", None),
        check_vma=False,
    )
```
